128 devices in a mesh: peer: 32 (over z_hi, x, y), zero: 4 (over z_lo, core).
Axes of the slice: x: 4, y: 4, z: 4 (z_hi: 2, z_lo: 2; z = z_hi * 2 + z_lo), core: 2. Of those that a mesh axis runs over, the one named last changes fastest.
Arguments:
- tokens: bfloat16 [32, 2048, 1024], P('peer', 'zero'), may hold values from -6 to 6
- out_grad: bfloat16 [32, 2048, 1024], P('peer', 'zero'), may hold values from -6 to 6
- step: int32 [1], replicated, may hold values from 0 to 3999
- up_param: float32 [32, 1024, 2048], P('peer', 'zero'), may hold values from -0.2 to 0.2
- down_param: float32 [32, 2048, 1024], P('peer', 'zero'), may hold values from -0.2 to 0.2
- up_first: float32 [32, 1024, 2048], P('peer', 'zero'), may hold values from -27.1529 to 27.1529
- down_first: float32 [32, 2048, 1024], P('peer', 'zero'), may hold values from -27.1529 to 27.1529
- up_second: float32 [32, 1024, 2048], P('peer', 'zero'), may hold values from 0.8192 to 819.2
- down_second: float32 [32, 2048, 1024], P('peer', 'zero'), may hold values from 0.8192 to 819.2
Outputs:
- new_up: float32 [32, 1024, 2048], P('peer', 'zero')
- new_down: float32 [32, 2048, 1024], P('peer', 'zero')
- new_up_first: float32 [32, 1024, 2048], P('peer', 'zero')
- new_down_first: float32 [32, 2048, 1024], P('peer', 'zero')
- new_up_second: float32 [32, 1024, 2048], P('peer', 'zero')
- new_down_second: float32 [32, 2048, 1024], P('peer', 'zero')
The draws below stay inside these ranges and needn't reach their ends.
All inputs are finite; a program needn't handle non-finite values.
Results may differ from the reference program's by a relative error of at most 0.0065.
Values may be sent and summed in bfloat16 or wider, within the bound.
No kernel may reach another device: no remote copies, remote signals or barrier semaphores. Data moves between devices by JAX's collectives and lax.ppermute only.
A program may use at most 128 MiB of HBM per device.

```python
import math
import jax
import jax.numpy as jnp
from jax import lax

D = 1024
FFW = 2048
GTOK = 2048
GROUPS = 32
N_PEER = 32


def block_levels(key, shape, cuts, low, high):
    level = 1.0
    for position, blocks in cuts:
        steps = jax.random.uniform(jax.random.fold_in(jax.random.fold_in(key, 6), position), (blocks,), jnp.float32, low / len(cuts), high / len(cuts))
        level = level * jnp.repeat(jnp.exp(steps), shape[position] // blocks).reshape((-1,) + (1,) * (len(shape) - 1 - position))
    return level


def scatter_about(own_key, shape, width, limit, pieces=(), held_as=jnp.bfloat16):
    values = width * jax.random.normal(own_key, shape, jnp.float32)
    if pieces:
        values = values * block_levels(own_key, shape, pieces, -0.22, 0.18)
    return jnp.clip(values, -limit, limit).astype(held_as)


def setup_inputs(seed: int = 0) -> dict:
    splits = jax.random.split(jax.random.key(seed), 10)
    tokens = scatter_about(splits[0], (GROUPS, GTOK, D), 1.0, 6.0, ((0, 32), (1, 4)))
    out_grad = scatter_about(splits[1], (GROUPS, GTOK, D), 1.0, 6.0, ((0, 32), (1, 4)))
    step = jax.random.randint(splits[2], (1,), 0, 4000).astype(jnp.int32)
    up_param = scatter_about(splits[3], (GROUPS, D, FFW), 0.03, 0.2, ((0, 32), (1, 4)), jnp.float32)
    down_param = scatter_about(splits[4], (GROUPS, FFW, D), 0.03, 0.2, ((0, 32), (1, 4)), jnp.float32)
    up_first = scatter_about(splits[5], (GROUPS, D, FFW), (0.1 * GTOK ** 0.5), 27.1529, ((0, 32), (1, 4)), jnp.float32)
    down_first = scatter_about(splits[6], (GROUPS, FFW, D), (0.1 * GTOK ** 0.5), 27.1529, ((0, 32), (1, 4)), jnp.float32)
    up_second = jnp.clip(jnp.exp(math.log(819.2) - 6.9077553 * jax.random.uniform(splits[7], (GROUPS, D, FFW), jnp.float32) ** block_levels(splits[7], (GROUPS, D, FFW), ((0, 32), (1, 4)), -0.2, 0.2)), 0.8192, 819.2)
    down_second = jnp.clip(jnp.exp(math.log(819.2) - 6.9077553 * jax.random.uniform(splits[8], (GROUPS, FFW, D), jnp.float32) ** block_levels(splits[8], (GROUPS, FFW, D), ((0, 32), (1, 4)), -0.2, 0.2)), 0.8192, 819.2)
    return {"tokens": tokens, "out_grad": out_grad, "step": step, "up_param": up_param, "down_param": down_param, "up_first": up_first, "down_first": down_first, "up_second": up_second, "down_second": down_second}


def gelu_tanh(values):
    return 0.5 * values * (1.0 + jnp.tanh(0.7978845608 * (values + 0.044715 * values * values * values)))

def group_grads(items):
    tokens, out_grad, up_param, down_param = items
    widened = tokens.astype(jnp.float32)
    center = lax.optimization_barrier(jnp.mean(widened, axis=1, keepdims=True))
    spread = lax.optimization_barrier(jnp.mean((widened - center) * (widened - center), axis=1, keepdims=True))
    normed = ((widened - center) * lax.rsqrt(spread + 1e-05)).astype(jnp.bfloat16)
    up_low = up_param.astype(jnp.bfloat16)
    down_low = down_param.astype(jnp.bfloat16)
    pre = jnp.dot(normed, up_low, preferred_element_type=jnp.float32)
    active, backward = jax.vjp(gelu_tanh, pre)
    act = active.astype(jnp.bfloat16)
    act_grad = jnp.dot(out_grad, down_low.T, preferred_element_type=jnp.float32)
    pre_grad = backward(act_grad)[0].astype(jnp.bfloat16)
    up_grad = jnp.dot(normed.T, pre_grad, preferred_element_type=jnp.float32)
    down_grad = jnp.dot(act.T, out_grad, preferred_element_type=jnp.float32)
    return (up_grad, down_grad)

def adam_update(param, first, second, grad, first_fix, second_fix):
    first_new = 0.9 * first + 0.1 * grad
    second_new = 0.999 * second + 0.001 * grad * grad
    local = param - 0.01 * (first_new / first_fix) / (jnp.sqrt(second_new / second_fix) + 1e-08)
    return (local, first_new, second_new)

def reference(tokens, out_grad, step, up_param, down_param, up_first, down_first, up_second, down_second):
    up_grad, down_grad = lax.map(group_grads, (tokens, out_grad, up_param, down_param))
    count = (step[0] + 1).astype(jnp.float32)
    first_fix = 1.0 - jnp.power(jnp.float32(0.9), count)
    second_fix = 1.0 - jnp.power(jnp.float32(0.999), count)
    up_local, up_first_new, up_second_new = adam_update(up_param, up_first, up_second, up_grad, first_fix, second_fix)
    down_local, down_first_new, down_second_new = adam_update(down_param, down_first, down_second, down_grad, first_fix, second_fix)
    levels = N_PEER.bit_length() - 1
    distance = jnp.left_shift(jnp.int32(1), (step[0] % levels).astype(jnp.int32))
    partner = ((jnp.arange(N_PEER, dtype=jnp.int32) + distance) % N_PEER).astype(jnp.int32)
    new_up = 0.5 * (up_local + jnp.take(up_local, partner, axis=0))
    new_down = 0.5 * (down_local + jnp.take(down_local, partner, axis=0))
    return (new_up, new_down, up_first_new, down_first_new, up_second_new, down_second_new)
```

```python
from functools import partial

import jax
import jax.numpy as jnp
from jax import lax
from jax.experimental import pallas as pl
from jax.experimental.pallas import tpu as pltpu
from jax.sharding import PartitionSpec as P


WIDTHS = (640, 384)
STARTS = tuple(sum(WIDTHS[:c]) for c in range(len(WIDTHS)))
CHUNKS = len(WIDTHS)
LOW = jnp.bfloat16
WIDE = jnp.float32
VMEM = pl.BlockSpec(memory_space=pltpu.VMEM)
HBM = pl.BlockSpec(memory_space=pltpu.HBM)
ANY = pl.BlockSpec(memory_space=pl.ANY)
SMEM = pl.BlockSpec(memory_space=pltpu.SMEM)
LIMIT = 20 * 2**20


def shape(*sizes, dtype=LOW):
    return jax.ShapeDtypeStruct(sizes, dtype)


def params(limit=LIMIT):
    return pltpu.CompilerParams(vmem_limit_bytes=limit)


def swap(array, mask):
    size = lax.axis_size("zero")
    return lax.ppermute(array, "zero", [(i, i ^ mask) for i in range(size)])


def from_partner(array, by):
    size = lax.axis_size("peer")
    return lax.ppermute(array, "peer", [(i, (i - by) % size) for i in range(size)])


def dot(left, right, over=((1,), (0,))):
    return lax.dot_general(left, right, (over, ((), ())), preferred_element_type=WIDE)


def adam(param, first, second, grad, fixes):
    first_new = 0.9 * first + 0.1 * grad
    second_new = 0.999 * second + 0.001 * grad * grad
    scaled = first_new * (0.01 / fixes[0])
    local = param - scaled / (jnp.sqrt(second_new * (1.0 / fixes[1])) + 1e-08)
    return local, first_new, second_new


def cut_kernel(place, up, *outs):
    step = 32
    width = outs[0].shape[1]

    def rows(i, _):
        at = pl.ds(pl.multiple_of(i * step, step), step)
        for k in range(4):
            col = pl.multiple_of((place[0] ^ k) * width, width)
            outs[k][at, :] = up[at, pl.ds(col, width)].astype(LOW)
        return 0

    lax.fori_loop(0, up.shape[0] // step, rows, 0)


def cut(place, up):
    return pl.pallas_call(
        cut_kernel,
        out_shape=[shape(up.shape[0], up.shape[1] // 4)] * 4,
        in_specs=[SMEM, VMEM],
        out_specs=[VMEM] * 4,
        compiler_params=params(),
        name="cut",
    )(place, up)


def norm_kernel(tokens, grads, _, normed, *pieces):
    step = 64

    def rows(i, _):
        at = pl.ds(pl.multiple_of(i * step, step), step)
        wide = tokens[at, :].astype(WIDE)
        centered = wide - jnp.mean(wide, axis=1, keepdims=True)
        spread = jnp.mean(centered * centered, axis=1, keepdims=True)
        normed[at, :] = (centered * lax.rsqrt(spread + 1e-05)).astype(LOW)
        for c, piece in enumerate(pieces):
            piece[at, :] = grads[at, STARTS[c] : STARTS[c] + WIDTHS[c]]
        return 0

    lax.fori_loop(0, tokens.shape[0] // step, rows, 0)


def norm(tokens, grads, after):
    rows, cols = tokens.shape
    return pl.pallas_call(
        norm_kernel,
        out_shape=[shape(rows, cols)] + [shape(rows, width) for width in WIDTHS],
        in_specs=[VMEM] * 2 + [ANY],
        out_specs=[VMEM] * (1 + CHUNKS),
        compiler_params=params(),
        name="norm",
    )(tokens, grads, after)


def hidden_kernel(place, u0, u1, u2, u3, left, right, act, slope, up, both):
    size = u0.shape[0]
    for k, u in enumerate((u0, u1, u2, u3)):
        up[pl.ds(pl.multiple_of((place[0] ^ k) * size, size), size), :] = u[...]
    half = left.shape[0]
    both[:half, :] = left[...]
    both[half:, :] = right[...]
    step = 256

    def rows(i, _):
        at = pl.ds(pl.multiple_of(i * step, step), step)
        pre = dot(both[at, :], up[...])
        square = pre * pre
        bent = jnp.tanh(0.7978845608 * (pre + 0.044715 * square * pre))
        lift = 0.5 * (1.0 + bent)
        act[:, at] = (pre * lift).T.astype(LOW)
        slope[at, :] = lift + 0.5 * pre * (1.0 - bent * bent) * (
            0.7978845608 + 0.1070322243 * square
        )
        return 0

    lax.fori_loop(0, 2 * half // step, rows, 0)


def hidden(place, ups, left, right):
    rows, full = left.shape
    width = ups[0].shape[1]
    return pl.pallas_call(
        hidden_kernel,
        out_shape=[shape(width, 2 * rows), shape(2 * rows, width, dtype=WIDE)],
        in_specs=[SMEM] + [VMEM] * 6,
        out_specs=[VMEM] * 2,
        scratch_shapes=[pltpu.VMEM((full, width), LOW), pltpu.VMEM((2 * rows, full), LOW)],
        compiler_params=params(),
        name="hidden",
    )(place, *ups, left, right)


def down_kernel(c, fixes, near, far, o0, o1, o2, o3, param, first, second, *rest):
    wholes, kept, (p, m, v, sems) = rest[-12:-8], rest[-8:-4], rest[-4:]
    local, send, mn, vn = kept
    cols = pl.ds(STARTS[c], WIDTHS[c])
    loads = [
        pltpu.make_async_copy(whole.at[:, cols], part, sems.at[i])
        for i, (whole, part) in enumerate(((param, p), (first, m), (second, v)))
    ]
    for load in loads:
        load.start()
    rows = o0.shape[0]
    local[...] = dot(near[:, :rows], o0[...])
    local[...] += dot(near[:, rows:], o1[:, STARTS[c] : STARTS[c] + WIDTHS[c]])
    local[...] += dot(far[:, :rows], o2[...])
    local[...] += dot(far[:, rows:], o3[...])
    for load in loads:
        load.wait()
    step = 64

    def some(i, _):
        at = pl.ds(pl.multiple_of(i * step, step), step)
        after, mn[at, :], vn[at, :] = adam(p[at, :], m[at, :], v[at, :], local[at, :], fixes)
        local[at, :] = after
        send[at, :] = after.astype(LOW)
        return 0

    lax.fori_loop(0, rows // step, some, 0)
    stores = [
        pltpu.make_async_copy(part, whole.at[:, cols], sems.at[i])
        for i, (whole, part) in enumerate(zip(wholes, kept))
    ]
    for store in stores:
        store.start()
    for store in stores:
        store.wait()


def down(c, fixes, near, far, ogs, param, first, second, news, after):
    rows, cols = param.shape
    part = (rows, WIDTHS[c])
    ins = [fixes, near, far, *ogs, param, first, second, after]
    in_specs = [SMEM] + [VMEM] * 6 + [HBM] * 3 + [ANY]
    aliases = {}
    if news is not None:
        aliases = {len(ins) + i: i for i in range(4)}
        ins += news
        in_specs += [HBM] * 4
    kinds = (WIDE, LOW, WIDE, WIDE)
    return pl.pallas_call(
        partial(down_kernel, c),
        out_shape=[shape(rows, cols, dtype=kind) for kind in kinds],
        in_specs=in_specs,
        out_specs=[HBM] * 4,
        input_output_aliases=aliases,
        scratch_shapes=[pltpu.VMEM(part, kind) for kind in kinds + (WIDE,) * 3]
        + [pltpu.SemaphoreType.DMA((4,))],
        compiler_params=params(),
        name="down",
    )(*ins)


def back_kernel(place, param, sa, sb, *refs):
    ogs, side, outs = refs[: 3 * CHUNKS], refs[3 * CHUNKS], refs[-6:-2]
    normed = refs[3 * CHUNKS + 1 : 3 * CHUNKS + 5]
    low, pre_grad = refs[-2:]
    rows = normed[0].shape[0]
    low[...] = param[...].astype(LOW)
    for k in range(4):
        got = None
        for c in range(CHUNKS):
            cols = slice(STARTS[c], STARTS[c] + WIDTHS[c])
            piece = side[:, cols] if k == 1 else ogs[(0, 0, 1, 2)[k] * CHUNKS + c][...]
            part = dot(piece, low[:, cols], ((1,), (1,)))
            got = part if got is None else got + part
        slope = (sa, sb)[k // 2][(k % 2) * rows : (k % 2 + 1) * rows, :]
        pre_grad[k * rows : (k + 1) * rows, :] = (got * slope).astype(LOW)
    size = outs[0].shape[0]
    for k in range(4):
        at = pl.ds(pl.multiple_of((place[0] ^ k) * size, size), size)
        total = None
        for j in range(4):
            part = dot(normed[j][:, at], pre_grad[j * rows : (j + 1) * rows, :], ((0,), (0,)))
            total = part if total is None else total + part
        outs[k][...] = total.astype(LOW)


def back(place, param, slopes, own, side, far, last, normed):
    hidden_size = param.shape[0]
    rows, full = normed[0].shape
    return pl.pallas_call(
        back_kernel,
        out_shape=[shape(full // 4, hidden_size)] * 4,
        in_specs=[SMEM] + [VMEM] * (3 + 3 * CHUNKS + 5),
        out_specs=[VMEM] * 4,
        scratch_shapes=[pltpu.VMEM(param.shape, LOW), pltpu.VMEM((4 * rows, hidden_size), LOW)],
        compiler_params=params(),
        name="back",
    )(place, param, *slopes, *own, *far, *last, side, *normed)


def up_kernel(base, place, fixes, left, right, param, first, second, *rest):
    local, send, first_new, second_new, p, m, v, mn, vn, sems = rest[-10:]
    rows, width = left.shape
    cols = [
        pl.ds(pl.multiple_of((place[0] ^ (base + i)) * width, width), width) for i in range(2)
    ]
    loads = [
        [
            pltpu.make_async_copy(whole.at[:, cols[i]], part.at[i], sems.at[3 * i + j])
            for j, (whole, part) in enumerate(((param, p), (first, m), (second, v)))
        ]
        for i in range(2)
    ]
    for load in loads[0] + loads[1]:
        load.start()
    stores = []
    step = 32
    for i, grads in enumerate((left, right)):
        for load in loads[i]:
            load.wait()

        def some(r, _):
            at = pl.ds(pl.multiple_of(r * step, step), step)
            to = pl.ds(pl.multiple_of(i * rows + r * step, step), step)
            after, mn[i, at, :], vn[i, at, :] = adam(
                p[i, at, :], m[i, at, :], v[i, at, :], grads[at, :].astype(WIDE), fixes
            )
            local[to, :] = after
            send[to, :] = after.astype(LOW)
            return 0

        lax.fori_loop(0, rows // step, some, 0)
        stores += [
            pltpu.make_async_copy(part.at[i], whole.at[:, cols[i]], sems.at[6 + 2 * i + j])
            for j, (whole, part) in enumerate(((first_new, mn), (second_new, vn)))
        ]
        for store in stores[-2:]:
            store.start()
    for store in stores:
        store.wait()


def up(base, place, fixes, left, right, param, first, second, news):
    rows, width = left.shape
    ins = [place, fixes, left, right, param, first, second]
    in_specs = [SMEM, SMEM, VMEM, VMEM, HBM, HBM, HBM]
    aliases = {}
    if news is not None:
        aliases = {len(ins): 2, len(ins) + 1: 3}
        ins += news
        in_specs += [HBM] * 2
    return pl.pallas_call(
        partial(up_kernel, base),
        in_specs=in_specs,
        out_specs=[VMEM, VMEM, HBM, HBM],
        out_shape=[
            shape(2 * rows, width, dtype=WIDE),
            shape(2 * rows, width),
            shape(*param.shape, dtype=WIDE),
            shape(*param.shape, dtype=WIDE),
        ],
        scratch_shapes=[pltpu.VMEM((2, rows, width), WIDE)] * 5
        + [pltpu.SemaphoreType.DMA((10,))],
        input_output_aliases=aliases,
        compiler_params=params(),
        name="up",
    )(*ins)


def mean_down_kernel(local, other, out):
    out[...] = 0.5 * (local[...] + other[...].astype(WIDE))


def mean_down(local, other):
    rows, cols = local.shape
    block = pl.BlockSpec((rows // 8, cols), lambda i: (i, 0))
    return pl.pallas_call(
        mean_down_kernel,
        grid=(8,),
        out_shape=shape(rows, cols, dtype=WIDE),
        in_specs=[block] * 2,
        out_specs=block,
        compiler_params=params(),
        name="mean_down",
    )(local, other)


def mean_up_kernel(base, place, local, other, *rest):
    out, kept, sems = rest[-3:]
    rows, width = kept.shape[1:]
    copies = []
    for i in range(2):
        kept[i] = 0.5 * (
            local[i * rows : (i + 1) * rows, :] + other[i * rows : (i + 1) * rows, :].astype(WIDE)
        )
        cols = pl.ds(pl.multiple_of((place[0] ^ (base + i)) * width, width), width)
        copies.append(pltpu.make_async_copy(kept.at[i], out.at[:, cols], sems.at[i]))
        copies[i].start()
    for copy in copies:
        copy.wait()


def mean_up(base, place, local, other, whole):
    rows, width = local.shape[0] // 2, local.shape[1]
    ins, in_specs, aliases = [place, local, other], [SMEM, VMEM, VMEM], {}
    if whole is not None:
        aliases = {3: 0}
        ins.append(whole)
        in_specs.append(HBM)
    return pl.pallas_call(
        partial(mean_up_kernel, base),
        in_specs=in_specs,
        out_specs=HBM,
        out_shape=shape(rows, 4 * width, dtype=WIDE),
        scratch_shapes=[pltpu.VMEM((2, rows, width), WIDE), pltpu.SemaphoreType.DMA((2,))],
        input_output_aliases=aliases,
        compiler_params=params(),
        name="mean_up",
    )(*ins)


def prepare(place, fixes, tokens, grads, up_p, down_p, up_m, down_m, up_v, down_v):
    first = cut(place, up_p)
    ups = [first[0]]
    for k in range(1, 4):
        ups.append(swap(first[k], k))
    n0, *own = norm(tokens, grads, first[0])
    n2 = swap(n0, 2)
    n1 = swap(n0, 1)
    side = swap(grads, 1)
    far, last = [], []
    for c in range(CHUNKS):
        far.append(swap(own[c], 2))
    near_act, near_slope = hidden(place, ups, n0, n1)
    n3 = swap(n2, 1)
    far_act, far_slope = hidden(place, ups, n2, n3)
    for c in range(CHUNKS):
        last.append(swap(far[c], 1))
    acts, slopes = (near_act, far_act), (near_slope, far_slope)
    news = None
    for c in range(CHUNKS - 1):
        ogs = (own[c], side, far[c], last[c])
        news = down(c, fixes, *acts, ogs, down_p, down_m, down_v, news, n0)
    g0, g1, g2, g3 = back(place, down_p, slopes, own, side, far, last, (n0, n1, n2, n3))
    g2 = swap(g2, 2)
    g3 = swap(g3, 3)
    g1 = swap(g1, 1)
    c = CHUNKS - 1
    ogs = (own[c], side, far[c], last[c])
    news = down(c, fixes, *acts, ogs, down_p, down_m, down_v, news, g0)
    near = up(0, place, fixes, g0, g1, up_p, up_m, up_v, None)
    return news, near, g2, g3


def finish(level, place, fixes, made, up_p, up_m, up_v):
    by = 2**level
    (down_local, send, *down_new), (near_local, near_send, *up_new), g2, g3 = made
    other = from_partner(send, by)
    near_other = from_partner(near_send, by)
    far_local, send, *up_new = up(2, place, fixes, g2, g3, up_p, up_m, up_v, up_new)
    far_other = from_partner(send, by)
    new_down = mean_down(down_local, other)
    new_up = mean_up(0, place, near_local, near_other, None)
    new_up = mean_up(2, place, far_local, far_other, new_up)
    return new_up, new_down, up_new[0], down_new[0], up_new[1], down_new[1]


def body(tokens, out_grad, step, *state):
    levels = lax.axis_size("peer").bit_length() - 1
    place = lax.axis_index("zero").astype(jnp.int32)[None]
    state = [a[0] for a in state]
    count = (step[0] + 1).astype(WIDE)
    fixes = jnp.stack(
        [1.0 - jnp.power(WIDE(0.9), count), 1.0 - jnp.power(WIDE(0.999), count)]
    )
    made = prepare(place, fixes, tokens[0], out_grad[0], *state)

    def branch(k, *args):
        return finish(k, *args)

    outs = lax.switch(
        step[0] % levels,
        [partial(branch, k) for k in range(levels)],
        place,
        fixes,
        made,
        *state[::2],
    )
    return tuple(a[None] for a in outs)


def solution(mesh):
    in_specs = (P("peer", "zero", None), P("peer", "zero", None), P()) + (
        P("peer", "zero", None),
    ) * 6
    out_specs = (P("peer", "zero", None),) * 6
    return jax.shard_map(body, mesh=mesh, in_specs=in_specs, out_specs=out_specs, check_vma=False)
```

```python
from functools import partial

import jax
import jax.numpy as jnp
from jax import lax
from jax.experimental import pallas as pl
from jax.experimental.pallas import tpu as pltpu
from jax.sharding import PartitionSpec as P


WIDTHS = (512, 512)
STARTS = tuple(sum(WIDTHS[:c]) for c in range(len(WIDTHS)))
CHUNKS = len(WIDTHS)
LOW = jnp.bfloat16
WIDE = jnp.float32
VMEM = pl.BlockSpec(memory_space=pltpu.VMEM)
HBM = pl.BlockSpec(memory_space=pltpu.HBM)
ANY = pl.BlockSpec(memory_space=pl.ANY)
SMEM = pl.BlockSpec(memory_space=pltpu.SMEM)
LIMIT = 20 * 2**20


def shape(*sizes, dtype=LOW):
    return jax.ShapeDtypeStruct(sizes, dtype)


def params(limit=LIMIT):
    return pltpu.CompilerParams(vmem_limit_bytes=limit)


def swap(array, mask):
    size = lax.axis_size("zero")
    return lax.ppermute(array, "zero", [(i, i ^ mask) for i in range(size)])


def from_partner(array, by):
    size = lax.axis_size("peer")
    return lax.ppermute(array, "peer", [(i, (i - by) % size) for i in range(size)])


def dot(left, right, over=((1,), (0,))):
    return lax.dot_general(left, right, (over, ((), ())), preferred_element_type=WIDE)


def adam(param, first, second, grad, fixes):
    first_new = 0.9 * first + 0.1 * grad
    second_new = 0.999 * second + 0.001 * grad * grad
    scaled = first_new * (0.01 / fixes[0])
    local = param - scaled / (jnp.sqrt(second_new * (1.0 / fixes[1])) + 1e-08)
    return local, first_new, second_new


def cut_kernel(place, up, *refs):
    outs = refs[-4:]
    step = 32
    width = outs[0].shape[1]

    def rows(i, _):
        at = pl.ds(pl.multiple_of(i * step, step), step)
        for k in range(4):
            col = pl.multiple_of((place[0] ^ k) * width, width)
            outs[k][at, :] = up[at, pl.ds(col, width)].astype(LOW)
        return 0

    lax.fori_loop(0, up.shape[0] // step, rows, 0)


def cut(place, up, *after):
    return pl.pallas_call(
        cut_kernel,
        out_shape=[shape(up.shape[0], up.shape[1] // 4)] * 4,
        in_specs=[SMEM, VMEM] + [ANY] * len(after),
        out_specs=[VMEM] * 4,
        compiler_params=params(),
        name="cut",
    )(place, up, *after)


def norm_kernel(tokens, grads, _, normed, *pieces):
    step = 64

    def rows(i, _):
        at = pl.ds(pl.multiple_of(i * step, step), step)
        wide = tokens[at, :].astype(WIDE)
        centered = wide - jnp.mean(wide, axis=1, keepdims=True)
        spread = jnp.mean(centered * centered, axis=1, keepdims=True)
        normed[at, :] = (centered * lax.rsqrt(spread + 1e-05)).astype(LOW)
        for c, piece in enumerate(pieces):
            piece[at, :] = grads[at, STARTS[c] : STARTS[c] + WIDTHS[c]]
        return 0

    lax.fori_loop(0, tokens.shape[0] // step, rows, 0)


def norm(tokens, grads, after):
    rows, cols = tokens.shape
    return pl.pallas_call(
        norm_kernel,
        out_shape=[shape(rows, cols)] + [shape(rows, width) for width in WIDTHS],
        in_specs=[VMEM] * 2 + [ANY],
        out_specs=[VMEM] * (1 + CHUNKS),
        compiler_params=params(),
        name="norm",
    )(tokens, grads, after)


def hidden_kernel(place, u0, u1, u2, u3, left, right, act, slope, up, both):
    size = u0.shape[0]
    for k, u in enumerate((u0, u1, u2, u3)):
        up[pl.ds(pl.multiple_of((place[0] ^ k) * size, size), size), :] = u[...]
    half = left.shape[0]
    both[:half, :] = left[...]
    both[half:, :] = right[...]
    step = 256

    def rows(i, _):
        at = pl.ds(pl.multiple_of(i * step, step), step)
        pre = dot(both[at, :], up[...])
        square = pre * pre
        bent = jnp.tanh(0.7978845608 * (pre + 0.044715 * square * pre))
        lift = 0.5 * (1.0 + bent)
        act[:, at] = (pre * lift).T.astype(LOW)
        slope[at, :] = lift + 0.5 * pre * (1.0 - bent * bent) * (
            0.7978845608 + 0.1070322243 * square
        )
        return 0

    lax.fori_loop(0, 2 * half // step, rows, 0)


def hidden(place, ups, left, right):
    rows, full = left.shape
    width = ups[0].shape[1]
    return pl.pallas_call(
        hidden_kernel,
        out_shape=[shape(width, 2 * rows), shape(2 * rows, width, dtype=WIDE)],
        in_specs=[SMEM] + [VMEM] * 6,
        out_specs=[VMEM] * 2,
        scratch_shapes=[pltpu.VMEM((full, width), LOW), pltpu.VMEM((2 * rows, full), LOW)],
        compiler_params=params(),
        name="hidden",
    )(place, *ups, left, right)


def down_kernel(c, fixes, near, far, o0, o1, o2, o3, param, first, second, *rest):
    wholes, kept, (p, m, v, sems) = rest[-12:-8], rest[-8:-4], rest[-4:]
    local, send, mn, vn = kept
    cols = pl.ds(STARTS[c], WIDTHS[c])
    loads = [
        pltpu.make_async_copy(whole.at[:, cols], part, sems.at[i])
        for i, (whole, part) in enumerate(((param, p), (first, m), (second, v)))
    ]
    for load in loads:
        load.start()
    rows = o0.shape[0]
    local[...] = dot(near[:, :rows], o0[...])
    local[...] += dot(near[:, rows:], o1[:, STARTS[c] : STARTS[c] + WIDTHS[c]])
    local[...] += dot(far[:, :rows], o2[...])
    local[...] += dot(far[:, rows:], o3[...])
    for load in loads:
        load.wait()
    step = 64

    def some(i, _):
        at = pl.ds(pl.multiple_of(i * step, step), step)
        after, mn[at, :], vn[at, :] = adam(p[at, :], m[at, :], v[at, :], local[at, :], fixes)
        local[at, :] = after
        send[at, :] = after.astype(LOW)
        return 0

    lax.fori_loop(0, rows // step, some, 0)
    stores = [
        pltpu.make_async_copy(part, whole.at[:, cols], sems.at[i])
        for i, (whole, part) in enumerate(zip(wholes, kept))
    ]
    for store in stores:
        store.start()
    for store in stores:
        store.wait()


def down(c, fixes, near, far, ogs, param, first, second, news, after):
    rows, cols = param.shape
    part = (rows, WIDTHS[c])
    ins = [fixes, near, far, *ogs, param, first, second, after]
    in_specs = [SMEM] + [VMEM] * 6 + [HBM] * 3 + [ANY]
    aliases = {}
    if news is not None:
        aliases = {len(ins) + i: i for i in range(4)}
        ins += news
        in_specs += [HBM] * 4
    kinds = (WIDE, LOW, WIDE, WIDE)
    return pl.pallas_call(
        partial(down_kernel, c),
        out_shape=[shape(rows, cols, dtype=kind) for kind in kinds],
        in_specs=in_specs,
        out_specs=[HBM] * 4,
        input_output_aliases=aliases,
        scratch_shapes=[pltpu.VMEM(part, kind) for kind in kinds + (WIDE,) * 3]
        + [pltpu.SemaphoreType.DMA((4,))],
        compiler_params=params(),
        name="down",
    )(*ins)


def back_kernel(place, param, sa, sb, *refs):
    ogs, side, outs = refs[: 3 * CHUNKS], refs[3 * CHUNKS], refs[-6:-2]
    normed = refs[3 * CHUNKS + 1 : 3 * CHUNKS + 5]
    low, pre_grad = refs[-2:]
    rows = normed[0].shape[0]
    low[...] = param[...].astype(LOW)
    for k in range(4):
        got = None
        for c in range(CHUNKS):
            cols = slice(STARTS[c], STARTS[c] + WIDTHS[c])
            piece = side[:, cols] if k == 1 else ogs[(0, 0, 1, 2)[k] * CHUNKS + c][...]
            part = dot(piece, low[:, cols], ((1,), (1,)))
            got = part if got is None else got + part
        slope = (sa, sb)[k // 2][(k % 2) * rows : (k % 2 + 1) * rows, :]
        pre_grad[k * rows : (k + 1) * rows, :] = (got * slope).astype(LOW)
    size = outs[0].shape[0]
    for k in range(4):
        at = pl.ds(pl.multiple_of((place[0] ^ k) * size, size), size)
        total = None
        for j in range(4):
            part = dot(normed[j][:, at], pre_grad[j * rows : (j + 1) * rows, :], ((0,), (0,)))
            total = part if total is None else total + part
        outs[k][...] = total.astype(LOW)


def back(place, param, slopes, own, side, far, last, normed):
    hidden_size = param.shape[0]
    rows, full = normed[0].shape
    return pl.pallas_call(
        back_kernel,
        out_shape=[shape(full // 4, hidden_size)] * 4,
        in_specs=[SMEM] + [VMEM] * (3 + 3 * CHUNKS + 5),
        out_specs=[VMEM] * 4,
        scratch_shapes=[pltpu.VMEM(param.shape, LOW), pltpu.VMEM((4 * rows, hidden_size), LOW)],
        compiler_params=params(),
        name="back",
    )(place, param, *slopes, *own, *far, *last, side, *normed)


def up_kernel(base, place, fixes, left, right, param, first, second, *rest):
    local, send, first_new, second_new, p, m, v, mn, vn, sems = rest[-10:]
    rows, width = left.shape
    cols = [
        pl.ds(pl.multiple_of((place[0] ^ (base + i)) * width, width), width) for i in range(2)
    ]
    loads = [
        [
            pltpu.make_async_copy(whole.at[:, cols[i]], part.at[i], sems.at[3 * i + j])
            for j, (whole, part) in enumerate(((param, p), (first, m), (second, v)))
        ]
        for i in range(2)
    ]
    for load in loads[0] + loads[1]:
        load.start()
    stores = []
    step = 32
    for i, grads in enumerate((left, right)):
        for load in loads[i]:
            load.wait()

        def some(r, _):
            at = pl.ds(pl.multiple_of(r * step, step), step)
            to = pl.ds(pl.multiple_of(i * rows + r * step, step), step)
            after, mn[i, at, :], vn[i, at, :] = adam(
                p[i, at, :], m[i, at, :], v[i, at, :], grads[at, :].astype(WIDE), fixes
            )
            local[to, :] = after
            send[to, :] = after.astype(LOW)
            return 0

        lax.fori_loop(0, rows // step, some, 0)
        stores += [
            pltpu.make_async_copy(part.at[i], whole.at[:, cols[i]], sems.at[6 + 2 * i + j])
            for j, (whole, part) in enumerate(((first_new, mn), (second_new, vn)))
        ]
        for store in stores[-2:]:
            store.start()
    for store in stores:
        store.wait()


def up(base, place, fixes, left, right, param, first, second, news):
    rows, width = left.shape
    ins = [place, fixes, left, right, param, first, second]
    in_specs = [SMEM, SMEM, VMEM, VMEM, HBM, HBM, HBM]
    aliases = {}
    if news is not None:
        aliases = {len(ins): 2, len(ins) + 1: 3}
        ins += news
        in_specs += [HBM] * 2
    return pl.pallas_call(
        partial(up_kernel, base),
        in_specs=in_specs,
        out_specs=[VMEM, VMEM, HBM, HBM],
        out_shape=[
            shape(2 * rows, width, dtype=WIDE),
            shape(2 * rows, width),
            shape(*param.shape, dtype=WIDE),
            shape(*param.shape, dtype=WIDE),
        ],
        scratch_shapes=[pltpu.VMEM((2, rows, width), WIDE)] * 5
        + [pltpu.SemaphoreType.DMA((10,))],
        input_output_aliases=aliases,
        compiler_params=params(),
        name="up",
    )(*ins)


def mean_down_kernel(local, other, out):
    out[...] = 0.5 * (local[...] + other[...].astype(WIDE))


def mean_down(local, other):
    rows, cols = local.shape
    block = pl.BlockSpec((rows // 8, cols), lambda i: (i, 0))
    return pl.pallas_call(
        mean_down_kernel,
        grid=(8,),
        out_shape=shape(rows, cols, dtype=WIDE),
        in_specs=[block] * 2,
        out_specs=block,
        compiler_params=params(60 * 2**20),
        name="mean_down",
    )(local, other)


def mean_up_kernel(base, place, local, other, *rest):
    out, kept, sems = rest[-3:]
    rows, width = kept.shape[1:]
    copies = []
    for i in range(2):
        kept[i] = 0.5 * (
            local[i * rows : (i + 1) * rows, :] + other[i * rows : (i + 1) * rows, :].astype(WIDE)
        )
        cols = pl.ds(pl.multiple_of((place[0] ^ (base + i)) * width, width), width)
        copies.append(pltpu.make_async_copy(kept.at[i], out.at[:, cols], sems.at[i]))
        copies[i].start()
    for copy in copies:
        copy.wait()


def mean_up(base, place, local, other, whole):
    rows, width = local.shape[0] // 2, local.shape[1]
    ins, in_specs, aliases = [place, local, other], [SMEM, VMEM, VMEM], {}
    if whole is not None:
        aliases = {3: 0}
        ins.append(whole)
        in_specs.append(HBM)
    return pl.pallas_call(
        partial(mean_up_kernel, base),
        in_specs=in_specs,
        out_specs=HBM,
        out_shape=shape(rows, 4 * width, dtype=WIDE),
        scratch_shapes=[pltpu.VMEM((2, rows, width), WIDE), pltpu.SemaphoreType.DMA((2,))],
        input_output_aliases=aliases,
        compiler_params=params(),
        name="mean_up",
    )(*ins)


def prepare(place, fixes, level, tokens, grads, up_p, down_p, up_m, down_m, up_v, down_v):
    first = cut(place, up_p, fixes, level)
    ups = [first[0]]
    for k in range(1, 4):
        ups.append(swap(first[k], k))
    n0, *own = norm(tokens, grads, first[0])
    n2 = swap(n0, 2)
    n1 = swap(n0, 1)
    side = swap(grads, 1)
    far, last = [], []
    for c in range(CHUNKS):
        far.append(swap(own[c], 2))
    near_act, near_slope = hidden(place, ups, n0, n1)
    n3 = swap(n2, 1)
    far_act, far_slope = hidden(place, ups, n2, n3)
    for c in range(CHUNKS):
        last.append(swap(far[c], 1))
    acts, slopes = (near_act, far_act), (near_slope, far_slope)
    news = None
    for c in range(CHUNKS - 1):
        ogs = (own[c], side, far[c], last[c])
        news = down(c, fixes, *acts, ogs, down_p, down_m, down_v, news, n0)
    g0, g1, g2, g3 = back(place, down_p, slopes, own, side, far, last, (n0, n1, n2, n3))
    g2 = swap(g2, 2)
    g3 = swap(g3, 3)
    g1 = swap(g1, 1)
    c = CHUNKS - 1
    ogs = (own[c], side, far[c], last[c])
    news = down(c, fixes, *acts, ogs, down_p, down_m, down_v, news, g0)
    near = up(0, place, fixes, g0, g1, up_p, up_m, up_v, None)
    return news, near, g2, g3


def finish(level, place, fixes, made, up_p, up_m, up_v):
    by = 2**level
    (down_local, send, *down_new), (near_local, near_send, *up_new), g2, g3 = made
    other = from_partner(send, by)
    near_other = from_partner(near_send, by)
    far_local, send, *up_new = up(2, place, fixes, g2, g3, up_p, up_m, up_v, up_new)
    far_other = from_partner(send, by)
    new_down = mean_down(down_local, other)
    new_up = mean_up(0, place, near_local, near_other, None)
    new_up = mean_up(2, place, far_local, far_other, new_up)
    return new_up, new_down, up_new[0], down_new[0], up_new[1], down_new[1]


def body(tokens, out_grad, step, *state):
    levels = lax.axis_size("peer").bit_length() - 1
    place = lax.axis_index("zero").astype(jnp.int32)[None]
    state = [a[0] for a in state]
    count = (step[0] + 1).astype(WIDE)
    fixes = jnp.stack(
        [1.0 - jnp.power(WIDE(0.9), count), 1.0 - jnp.power(WIDE(0.999), count)]
    )
    level = step % levels
    made = prepare(place, fixes, level, tokens[0], out_grad[0], *state)

    def branch(k, *args):
        return finish(k, *args)

    outs = lax.switch(
        level[0],
        [partial(branch, k) for k in range(levels)],
        place,
        fixes,
        made,
        *state[::2],
    )
    return tuple(a[None] for a in outs)


def solution(mesh):
    in_specs = (P("peer", "zero", None), P("peer", "zero", None), P()) + (
        P("peer", "zero", None),
    ) * 6
    out_specs = (P("peer", "zero", None),) * 6
    return jax.shard_map(body, mesh=mesh, in_specs=in_specs, out_specs=out_specs, check_vma=False)
```

```python
from functools import partial

import jax
import jax.numpy as jnp
from jax import lax
from jax.experimental import pallas as pl
from jax.experimental.pallas import tpu as pltpu
from jax.sharding import PartitionSpec as P


WIDTHS = (640, 384)
STARTS = tuple(sum(WIDTHS[:c]) for c in range(len(WIDTHS)))
CHUNKS = len(WIDTHS)
LOW = jnp.bfloat16
WIDE = jnp.float32
VMEM = pl.BlockSpec(memory_space=pltpu.VMEM)
HBM = pl.BlockSpec(memory_space=pltpu.HBM)
ANY = pl.BlockSpec(memory_space=pl.ANY)
SMEM = pl.BlockSpec(memory_space=pltpu.SMEM)
LIMIT = 20 * 2**20


def shape(*sizes, dtype=LOW):
    return jax.ShapeDtypeStruct(sizes, dtype)


def params(limit=LIMIT):
    return pltpu.CompilerParams(vmem_limit_bytes=limit)


def swap(array, mask):
    size = lax.axis_size("zero")
    return lax.ppermute(array, "zero", [(i, i ^ mask) for i in range(size)])


def from_partner(array, by):
    size = lax.axis_size("peer")
    return lax.ppermute(array, "peer", [(i, (i - by) % size) for i in range(size)])


def dot(left, right, over=((1,), (0,))):
    return lax.dot_general(left, right, (over, ((), ())), preferred_element_type=WIDE)


def adam(param, first, second, grad, fixes):
    first_new = 0.9 * first + 0.1 * grad
    second_new = 0.999 * second + 0.001 * grad * grad
    scaled = first_new * (0.01 / fixes[0])
    local = param - scaled / (jnp.sqrt(second_new * (1.0 / fixes[1])) + 1e-08)
    return local, first_new, second_new


def cut_kernel(place, up, *refs):
    outs = refs[-4:]
    step = 32
    width = outs[0].shape[1]

    def rows(i, _):
        at = pl.ds(pl.multiple_of(i * step, step), step)
        for k in range(4):
            col = pl.multiple_of((place[0] ^ k) * width, width)
            outs[k][at, :] = up[at, pl.ds(col, width)].astype(LOW)
        return 0

    lax.fori_loop(0, up.shape[0] // step, rows, 0)


def cut(place, up, *after):
    return pl.pallas_call(
        cut_kernel,
        out_shape=[shape(up.shape[0], up.shape[1] // 4)] * 4,
        in_specs=[SMEM, VMEM] + [ANY] * len(after),
        out_specs=[VMEM] * 4,
        compiler_params=params(),
        name="cut",
    )(place, up, *after)


def norm_kernel(tokens, grads, _, normed, *pieces):
    step = 64

    def rows(i, _):
        at = pl.ds(pl.multiple_of(i * step, step), step)
        wide = tokens[at, :].astype(WIDE)
        centered = wide - jnp.mean(wide, axis=1, keepdims=True)
        spread = jnp.mean(centered * centered, axis=1, keepdims=True)
        normed[at, :] = (centered * lax.rsqrt(spread + 1e-05)).astype(LOW)
        for c, piece in enumerate(pieces):
            piece[at, :] = grads[at, STARTS[c] : STARTS[c] + WIDTHS[c]]
        return 0

    lax.fori_loop(0, tokens.shape[0] // step, rows, 0)


def norm(tokens, grads, after):
    rows, cols = tokens.shape
    return pl.pallas_call(
        norm_kernel,
        out_shape=[shape(rows, cols)] + [shape(rows, width) for width in WIDTHS],
        in_specs=[VMEM] * 2 + [ANY],
        out_specs=[VMEM] * (1 + CHUNKS),
        compiler_params=params(),
        name="norm",
    )(tokens, grads, after)


def hidden_kernel(place, u0, u1, u2, u3, left, right, act, slope, up, both):
    size = u0.shape[0]
    for k, u in enumerate((u0, u1, u2, u3)):
        up[pl.ds(pl.multiple_of((place[0] ^ k) * size, size), size), :] = u[...]
    half = left.shape[0]
    both[:half, :] = left[...]
    both[half:, :] = right[...]
    step = 256

    def rows(i, _):
        at = pl.ds(pl.multiple_of(i * step, step), step)
        pre = dot(both[at, :], up[...])
        square = pre * pre
        bent = jnp.tanh(0.7978845608 * (pre + 0.044715 * square * pre))
        lift = 0.5 * (1.0 + bent)
        act[:, at] = (pre * lift).T.astype(LOW)
        slope[at, :] = lift + 0.5 * pre * (1.0 - bent * bent) * (
            0.7978845608 + 0.1070322243 * square
        )
        return 0

    lax.fori_loop(0, 2 * half // step, rows, 0)


def hidden(place, ups, left, right):
    rows, full = left.shape
    width = ups[0].shape[1]
    return pl.pallas_call(
        hidden_kernel,
        out_shape=[shape(width, 2 * rows), shape(2 * rows, width, dtype=WIDE)],
        in_specs=[SMEM] + [VMEM] * 6,
        out_specs=[VMEM] * 2,
        scratch_shapes=[pltpu.VMEM((full, width), LOW), pltpu.VMEM((2 * rows, full), LOW)],
        compiler_params=params(),
        name="hidden",
    )(place, *ups, left, right)


def down_kernel(c, fixes, near, far, o0, o1, o2, o3, param, first, second, *rest):
    wholes, send, kept, (p, m, v, sems) = rest[-11:-8], rest[-8], rest[-7:-4], rest[-4:]
    local, mn, vn = kept
    cols = pl.ds(STARTS[c], WIDTHS[c])
    loads = [
        pltpu.make_async_copy(whole.at[:, cols], part, sems.at[i])
        for i, (whole, part) in enumerate(((param, p), (first, m), (second, v)))
    ]
    for load in loads:
        load.start()
    rows = o0.shape[0]
    local[...] = dot(near[:, :rows], o0[...])
    local[...] += dot(near[:, rows:], o1[:, STARTS[c] : STARTS[c] + WIDTHS[c]])
    local[...] += dot(far[:, :rows], o2[...])
    local[...] += dot(far[:, rows:], o3[...])
    for load in loads:
        load.wait()
    step = 64

    def some(i, _):
        at = pl.ds(pl.multiple_of(i * step, step), step)
        after, mn[at, :], vn[at, :] = adam(p[at, :], m[at, :], v[at, :], local[at, :], fixes)
        local[at, :] = after
        send[at, :] = after.astype(LOW)
        return 0

    lax.fori_loop(0, rows // step, some, 0)
    stores = [
        pltpu.make_async_copy(part, whole.at[:, cols], sems.at[i])
        for i, (whole, part) in enumerate(zip(wholes, kept))
    ]
    for store in stores:
        store.start()
    for store in stores:
        store.wait()


def down(c, fixes, near, far, ogs, param, first, second, news, after):
    rows, cols = param.shape
    part = (rows, WIDTHS[c])
    ins = [fixes, near, far, *ogs, param, first, second, after]
    in_specs = [SMEM] + [VMEM] * 6 + [HBM] * 3 + [ANY]
    aliases = {}
    if news is not None:
        aliases = {len(ins) + i: i for i in range(3)}
        ins += news
        in_specs += [HBM] * 3
    return pl.pallas_call(
        partial(down_kernel, c),
        out_shape=[shape(rows, cols, dtype=WIDE)] * 3 + [shape(*part)],
        in_specs=in_specs,
        out_specs=[HBM] * 3 + [VMEM],
        input_output_aliases=aliases,
        scratch_shapes=[pltpu.VMEM(part, WIDE)] * 6 + [pltpu.SemaphoreType.DMA((3,))],
        compiler_params=params(),
        name="down",
    )(*ins)


def back_kernel(place, param, sa, sb, *refs):
    ogs, side, outs = refs[: 3 * CHUNKS], refs[3 * CHUNKS], refs[-7:-3]
    normed = refs[3 * CHUNKS + 1 : 3 * CHUNKS + 5]
    low, pre_grad, grads = refs[-3:]
    rows = normed[0].shape[0]
    low[...] = param[...].astype(LOW)
    for k in range(4):
        got = None
        for c in range(CHUNKS):
            cols = slice(STARTS[c], STARTS[c] + WIDTHS[c])
            piece = side[:, cols] if k == 1 else ogs[(0, 0, 1, 2)[k] * CHUNKS + c][...]
            part = dot(piece, low[:, cols], ((1,), (1,)))
            got = part if got is None else got + part
        slope = (sa, sb)[k // 2][(k % 2) * rows : (k % 2 + 1) * rows, :]
        pre_grad[k * rows : (k + 1) * rows, :] = (got * slope).astype(LOW)
    size = outs[0].shape[0]

    def block(k, _):
        at = pl.ds(pl.multiple_of((place[0] ^ k) * size, size), size)
        total = None
        for j in range(4):
            part = dot(normed[j][:, at], pre_grad[j * rows : (j + 1) * rows, :], ((0,), (0,)))
            total = part if total is None else total + part
        grads[k] = total.astype(LOW)
        return 0

    lax.fori_loop(0, 4, block, 0)
    for k in range(4):
        outs[k][...] = grads[k]


def back(place, param, slopes, own, side, far, last, normed):
    hidden_size = param.shape[0]
    rows, full = normed[0].shape
    return pl.pallas_call(
        back_kernel,
        out_shape=[shape(full // 4, hidden_size)] * 4,
        in_specs=[SMEM] + [VMEM] * (3 + 3 * CHUNKS + 5),
        out_specs=[VMEM] * 4,
        scratch_shapes=[pltpu.VMEM(param.shape, LOW), pltpu.VMEM((4 * rows, hidden_size), LOW), pltpu.VMEM((4, full // 4, hidden_size), LOW)],
        compiler_params=params(),
        name="back",
    )(place, param, *slopes, *own, *far, *last, side, *normed)


def up_kernel(base, place, fixes, left, right, param, first, second, *rest):
    local, send, first_new, second_new, p, m, v, mn, vn, sems = rest[-10:]
    rows, width = left.shape
    cols = [
        pl.ds(pl.multiple_of((place[0] ^ (base + i)) * width, width), width) for i in range(2)
    ]
    loads = [
        [
            pltpu.make_async_copy(whole.at[:, cols[i]], part.at[i], sems.at[3 * i + j])
            for j, (whole, part) in enumerate(((param, p), (first, m), (second, v)))
        ]
        for i in range(2)
    ]
    for load in loads[0] + loads[1]:
        load.start()
    stores = []
    step = 32
    for i, grads in enumerate((left, right)):
        for load in loads[i]:
            load.wait()

        def some(r, _):
            at = pl.ds(pl.multiple_of(r * step, step), step)
            to = pl.ds(pl.multiple_of(i * rows + r * step, step), step)
            after, mn[i, at, :], vn[i, at, :] = adam(
                p[i, at, :], m[i, at, :], v[i, at, :], grads[at, :].astype(WIDE), fixes
            )
            local[to, :] = after
            send[to, :] = after.astype(LOW)
            return 0

        lax.fori_loop(0, rows // step, some, 0)
        stores += [
            pltpu.make_async_copy(part.at[i], whole.at[:, cols[i]], sems.at[6 + 2 * i + j])
            for j, (whole, part) in enumerate(((first_new, mn), (second_new, vn)))
        ]
        for store in stores[-2:]:
            store.start()
    for store in stores:
        store.wait()


def up(base, place, fixes, left, right, param, first, second, news):
    rows, width = left.shape
    ins = [place, fixes, left, right, param, first, second]
    in_specs = [SMEM, SMEM, VMEM, VMEM, HBM, HBM, HBM]
    aliases = {}
    if news is not None:
        aliases = {len(ins): 2, len(ins) + 1: 3}
        ins += news
        in_specs += [HBM] * 2
    return pl.pallas_call(
        partial(up_kernel, base),
        in_specs=in_specs,
        out_specs=[VMEM, VMEM, HBM, HBM],
        out_shape=[
            shape(2 * rows, width, dtype=WIDE),
            shape(2 * rows, width),
            shape(*param.shape, dtype=WIDE),
            shape(*param.shape, dtype=WIDE),
        ],
        scratch_shapes=[pltpu.VMEM((2, rows, width), WIDE)] * 5
        + [pltpu.SemaphoreType.DMA((10,))],
        input_output_aliases=aliases,
        compiler_params=params(),
        name="up",
    )(*ins)


def mean_down_kernel(local, *refs):
    out = refs[-1]
    for c in range(CHUNKS):
        cols = slice(STARTS[c], STARTS[c] + WIDTHS[c])
        out[:, cols] = 0.5 * (local[:, cols] + refs[c][...].astype(WIDE))


def mean_down(local, others):
    rows, cols = local.shape
    block = pl.BlockSpec((rows // 8, cols), lambda i: (i, 0))
    return pl.pallas_call(
        mean_down_kernel,
        grid=(8,),
        out_shape=shape(rows, cols, dtype=WIDE),
        in_specs=[block] + [pl.BlockSpec((rows // 8, w), lambda i: (i, 0)) for w in WIDTHS],
        out_specs=block,
        compiler_params=params(60 * 2**20),
        name="mean_down",
    )(local, *others)


def mean_up_kernel(base, place, local, other, *rest):
    out, kept, sems = rest[-3:]
    rows, width = kept.shape[1:]
    copies = []
    for i in range(2):
        kept[i] = 0.5 * (
            local[i * rows : (i + 1) * rows, :] + other[i * rows : (i + 1) * rows, :].astype(WIDE)
        )
        cols = pl.ds(pl.multiple_of((place[0] ^ (base + i)) * width, width), width)
        copies.append(pltpu.make_async_copy(kept.at[i], out.at[:, cols], sems.at[i]))
        copies[i].start()
    for copy in copies:
        copy.wait()


def mean_up(base, place, local, other, whole):
    rows, width = local.shape[0] // 2, local.shape[1]
    ins, in_specs, aliases = [place, local, other], [SMEM, VMEM, VMEM], {}
    if whole is not None:
        aliases = {3: 0}
        ins.append(whole)
        in_specs.append(HBM)
    return pl.pallas_call(
        partial(mean_up_kernel, base),
        in_specs=in_specs,
        out_specs=HBM,
        out_shape=shape(rows, 4 * width, dtype=WIDE),
        scratch_shapes=[pltpu.VMEM((2, rows, width), WIDE), pltpu.SemaphoreType.DMA((2,))],
        input_output_aliases=aliases,
        compiler_params=params(),
        name="mean_up",
    )(*ins)


def prepare(place, fixes, level, tokens, grads, up_p, down_p, down_m, down_v):
    first = cut(place, up_p, fixes, level)
    ups = [first[0]]
    for k in range(1, 4):
        ups.append(swap(first[k], k))
    n0, *own = norm(tokens, grads, first[0])
    n2 = swap(n0, 2)
    n1 = swap(n0, 1)
    side = swap(grads, 1)
    far, last = [], []
    for c in range(CHUNKS):
        far.append(swap(own[c], 2))
    near_act, near_slope = hidden(place, ups, n0, n1)
    n3 = swap(n2, 1)
    far_act, far_slope = hidden(place, ups, n2, n3)
    for c in range(CHUNKS):
        last.append(swap(far[c], 1))
    acts, slopes = (near_act, far_act), (near_slope, far_slope)
    news, sends = None, []
    for c in range(CHUNKS - 1):
        ogs = (own[c], side, far[c], last[c])
        *news, send = down(c, fixes, *acts, ogs, down_p, down_m, down_v, news, n0)
        sends.append(send)
    return news, sends, acts, slopes, own, side, far, last, (n0, n1, n2, n3)


def finish(level, place, fixes, made, up_p, down_p, up_m, down_m, up_v, down_v):
    by = 2**level
    news, sends, acts, slopes, own, side, far, last, normed = made
    others = []
    for c, send in enumerate(sends):
        others.append(from_partner(send, by))
    g0, g1, g2, g3 = back(place, down_p, slopes, own, side, far, last, normed)
    g2 = swap(g2, 2)
    g3 = swap(g3, 3)
    g1 = swap(g1, 1)
    c = CHUNKS - 1
    ogs = (own[c], side, far[c], last[c])
    *news, send = down(c, fixes, *acts, ogs, down_p, down_m, down_v, news, g0)
    others.append(from_partner(send, by))
    near_local, send, *up_new = up(0, place, fixes, g0, g1, up_p, up_m, up_v, None)
    near_other = from_partner(send, by)
    far_local, send, *up_new = up(2, place, fixes, g2, g3, up_p, up_m, up_v, up_new)
    far_other = from_partner(send, by)
    new_down = mean_down(news[0], others)
    new_up = mean_up(0, place, near_local, near_other, None)
    new_up = mean_up(2, place, far_local, far_other, new_up)
    return new_up, new_down, up_new[0], news[1], up_new[1], news[2]


def body(tokens, out_grad, step, *state):
    levels = lax.axis_size("peer").bit_length() - 1
    place = lax.axis_index("zero").astype(jnp.int32)[None]
    state = [a[0] for a in state]
    count = (step[0] + 1).astype(WIDE)
    fixes = jnp.stack(
        [1.0 - jnp.power(WIDE(0.9), count), 1.0 - jnp.power(WIDE(0.999), count)]
    )
    level = step % levels
    made = prepare(
        place, fixes, level, tokens[0], out_grad[0], state[0], *state[1::2]
    )

    def branch(k, *args):
        return finish(k, *args)

    outs = lax.switch(
        level[0],
        [partial(branch, k) for k in range(levels)],
        place,
        fixes,
        made,
        *state,
    )
    return tuple(a[None] for a in outs)


def solution(mesh):
    in_specs = (P("peer", "zero", None), P("peer", "zero", None), P()) + (
        P("peer", "zero", None),
    ) * 6
    out_specs = (P("peer", "zero", None),) * 6
    return jax.shard_map(body, mesh=mesh, in_specs=in_specs, out_specs=out_specs, check_vma=False)
```

```python
from functools import partial

import jax
import jax.numpy as jnp
from jax import lax
from jax.experimental import pallas as pl
from jax.experimental.pallas import tpu as pltpu
from jax.sharding import PartitionSpec as P


WIDTHS = (384, 640)
STARTS = tuple(sum(WIDTHS[:c]) for c in range(len(WIDTHS)))
CHUNKS = len(WIDTHS)
LOW = jnp.bfloat16
WIDE = jnp.float32
VMEM = pl.BlockSpec(memory_space=pltpu.VMEM)
HBM = pl.BlockSpec(memory_space=pltpu.HBM)
ANY = pl.BlockSpec(memory_space=pl.ANY)
SMEM = pl.BlockSpec(memory_space=pltpu.SMEM)
LIMIT = 20 * 2**20


def shape(*sizes, dtype=LOW):
    return jax.ShapeDtypeStruct(sizes, dtype)


def params(limit=LIMIT):
    return pltpu.CompilerParams(vmem_limit_bytes=limit)


def swap(array, mask):
    size = lax.axis_size("zero")
    return lax.ppermute(array, "zero", [(i, i ^ mask) for i in range(size)])


def from_partner(array, by):
    size = lax.axis_size("peer")
    return lax.ppermute(array, "peer", [(i, (i - by) % size) for i in range(size)])


def dot(left, right, over=((1,), (0,))):
    return lax.dot_general(left, right, (over, ((), ())), preferred_element_type=WIDE)


def adam(param, first, second, grad, fixes):
    first_new = 0.9 * first + 0.1 * grad
    second_new = 0.999 * second + 0.001 * grad * grad
    scaled = first_new * (0.01 / fixes[0])
    local = param - scaled / (jnp.sqrt(second_new * (1.0 / fixes[1])) + 1e-08)
    return local, first_new, second_new


def cut_kernel(place, up, *refs):
    outs = refs[-4:]
    step = 32
    width = outs[0].shape[1]

    def rows(i, _):
        at = pl.ds(pl.multiple_of(i * step, step), step)
        for k in range(4):
            col = pl.multiple_of((place[0] ^ k) * width, width)
            outs[k][at, :] = up[at, pl.ds(col, width)].astype(LOW)
        return 0

    lax.fori_loop(0, up.shape[0] // step, rows, 0)


def cut(place, up, *after):
    return pl.pallas_call(
        cut_kernel,
        out_shape=[shape(up.shape[0], up.shape[1] // 4)] * 4,
        in_specs=[SMEM, VMEM] + [ANY] * len(after),
        out_specs=[VMEM] * 4,
        compiler_params=params(),
        name="cut",
    )(place, up, *after)


def norm_kernel(tokens, grads, _, normed, *pieces):
    step = 64

    def rows(i, _):
        at = pl.ds(pl.multiple_of(i * step, step), step)
        wide = tokens[at, :].astype(WIDE)
        centered = wide - jnp.mean(wide, axis=1, keepdims=True)
        spread = jnp.mean(centered * centered, axis=1, keepdims=True)
        normed[at, :] = (centered * lax.rsqrt(spread + 1e-05)).astype(LOW)
        for c, piece in enumerate(pieces):
            piece[at, :] = grads[at, STARTS[c] : STARTS[c] + WIDTHS[c]]
        return 0

    lax.fori_loop(0, tokens.shape[0] // step, rows, 0)


def norm(tokens, grads, after):
    rows, cols = tokens.shape
    return pl.pallas_call(
        norm_kernel,
        out_shape=[shape(rows, cols)] + [shape(rows, width) for width in WIDTHS],
        in_specs=[VMEM] * 2 + [ANY],
        out_specs=[VMEM] * (1 + CHUNKS),
        compiler_params=params(),
        name="norm",
    )(tokens, grads, after)


def hidden_kernel(place, u0, u1, u2, u3, left, right, act, slope, up, both):
    size = u0.shape[0]
    for k, u in enumerate((u0, u1, u2, u3)):
        up[pl.ds(pl.multiple_of((place[0] ^ k) * size, size), size), :] = u[...]
    half = left.shape[0]
    both[:half, :] = left[...]
    both[half:, :] = right[...]
    step = 256

    def rows(i, _):
        at = pl.ds(pl.multiple_of(i * step, step), step)
        pre = dot(both[at, :], up[...])
        square = pre * pre
        bent = jnp.tanh(0.7978845608 * (pre + 0.044715 * square * pre))
        lift = 0.5 * (1.0 + bent)
        act[:, at] = (pre * lift).T.astype(LOW)
        slope[at, :] = lift + 0.5 * pre * (1.0 - bent * bent) * (
            0.7978845608 + 0.1070322243 * square
        )
        return 0

    lax.fori_loop(0, 2 * half // step, rows, 0)


def hidden(place, ups, left, right):
    rows, full = left.shape
    width = ups[0].shape[1]
    return pl.pallas_call(
        hidden_kernel,
        out_shape=[shape(width, 2 * rows), shape(2 * rows, width, dtype=WIDE)],
        in_specs=[SMEM] + [VMEM] * 6,
        out_specs=[VMEM] * 2,
        scratch_shapes=[pltpu.VMEM((full, width), LOW), pltpu.VMEM((2 * rows, full), LOW)],
        compiler_params=params(),
        name="hidden",
    )(place, *ups, left, right)


def down_kernel(c, fixes, near, far, o0, o1, o2, o3, param, first, second, *rest):
    wholes, send, kept, (p, m, v, sems) = rest[-11:-8], rest[-8], rest[-7:-4], rest[-4:]
    local, mn, vn = kept
    cols = pl.ds(STARTS[c], WIDTHS[c])
    loads = [
        pltpu.make_async_copy(whole.at[:, cols], part, sems.at[i])
        for i, (whole, part) in enumerate(((param, p), (first, m), (second, v)))
    ]
    for load in loads:
        load.start()
    rows = o0.shape[0]
    local[...] = dot(near[:, :rows], o0[...])
    local[...] += dot(near[:, rows:], o1[:, STARTS[c] : STARTS[c] + WIDTHS[c]])
    local[...] += dot(far[:, :rows], o2[...])
    local[...] += dot(far[:, rows:], o3[...])
    for load in loads:
        load.wait()
    step = 64

    def some(i, _):
        at = pl.ds(pl.multiple_of(i * step, step), step)
        after, mn[at, :], vn[at, :] = adam(p[at, :], m[at, :], v[at, :], local[at, :], fixes)
        local[at, :] = after
        send[at, :] = after.astype(LOW)
        return 0

    lax.fori_loop(0, rows // step, some, 0)
    stores = [
        pltpu.make_async_copy(part, whole.at[:, cols], sems.at[i])
        for i, (whole, part) in enumerate(zip(wholes, kept))
    ]
    for store in stores:
        store.start()
    for store in stores:
        store.wait()


def down(c, fixes, near, far, ogs, param, first, second, news, after):
    rows, cols = param.shape
    part = (rows, WIDTHS[c])
    ins = [fixes, near, far, *ogs, param, first, second, after]
    in_specs = [SMEM] + [VMEM] * 6 + [HBM] * 3 + [ANY]
    aliases = {}
    if news is not None:
        aliases = {len(ins) + i: i for i in range(3)}
        ins += news
        in_specs += [HBM] * 3
    return pl.pallas_call(
        partial(down_kernel, c),
        out_shape=[shape(rows, cols, dtype=WIDE)] * 3 + [shape(*part)],
        in_specs=in_specs,
        out_specs=[HBM] * 3 + [VMEM],
        input_output_aliases=aliases,
        scratch_shapes=[pltpu.VMEM(part, WIDE)] * 6 + [pltpu.SemaphoreType.DMA((3,))],
        compiler_params=params(),
        name="down",
    )(*ins)


def back_kernel(place, param, sa, sb, *refs):
    ogs, side, outs = refs[: 3 * CHUNKS], refs[3 * CHUNKS], refs[-7:-3]
    normed = refs[3 * CHUNKS + 1 : 3 * CHUNKS + 5]
    low, pre_grad, grads = refs[-3:]
    rows = normed[0].shape[0]
    low[...] = param[...].astype(LOW)
    for k in range(4):
        got = None
        for c in range(CHUNKS):
            cols = slice(STARTS[c], STARTS[c] + WIDTHS[c])
            piece = side[:, cols] if k == 1 else ogs[(0, 0, 1, 2)[k] * CHUNKS + c][...]
            part = dot(piece, low[:, cols], ((1,), (1,)))
            got = part if got is None else got + part
        slope = (sa, sb)[k // 2][(k % 2) * rows : (k % 2 + 1) * rows, :]
        pre_grad[k * rows : (k + 1) * rows, :] = (got * slope).astype(LOW)
    size = outs[0].shape[0]

    def block(k, _):
        at = pl.ds(pl.multiple_of((place[0] ^ k) * size, size), size)
        total = None
        for j in range(4):
            part = dot(normed[j][:, at], pre_grad[j * rows : (j + 1) * rows, :], ((0,), (0,)))
            total = part if total is None else total + part
        grads[k] = total.astype(LOW)
        return 0

    lax.fori_loop(0, 4, block, 0)
    for k in range(4):
        outs[k][...] = grads[k]


def back(place, param, slopes, own, side, far, last, normed):
    hidden_size = param.shape[0]
    rows, full = normed[0].shape
    return pl.pallas_call(
        back_kernel,
        out_shape=[shape(full // 4, hidden_size)] * 4,
        in_specs=[SMEM] + [VMEM] * (3 + 3 * CHUNKS + 5),
        out_specs=[VMEM] * 4,
        scratch_shapes=[pltpu.VMEM(param.shape, LOW), pltpu.VMEM((4 * rows, hidden_size), LOW), pltpu.VMEM((4, full // 4, hidden_size), LOW)],
        compiler_params=params(),
        name="back",
    )(place, param, *slopes, *own, *far, *last, side, *normed)


def up_kernel(base, place, fixes, left, right, param, first, second, *rest):
    local, send, first_new, second_new, p, m, v, mn, vn, sems = rest[-10:]
    rows, width = left.shape
    cols = [
        pl.ds(pl.multiple_of((place[0] ^ (base + i)) * width, width), width) for i in range(2)
    ]
    loads = [
        [
            pltpu.make_async_copy(whole.at[:, cols[i]], part.at[i], sems.at[3 * i + j])
            for j, (whole, part) in enumerate(((param, p), (first, m), (second, v)))
        ]
        for i in range(2)
    ]
    for load in loads[0] + loads[1]:
        load.start()
    stores = []
    step = 32
    for i, grads in enumerate((left, right)):
        for load in loads[i]:
            load.wait()

        def some(r, _):
            at = pl.ds(pl.multiple_of(r * step, step), step)
            to = pl.ds(pl.multiple_of(i * rows + r * step, step), step)
            after, mn[i, at, :], vn[i, at, :] = adam(
                p[i, at, :], m[i, at, :], v[i, at, :], grads[at, :].astype(WIDE), fixes
            )
            local[to, :] = after
            send[to, :] = after.astype(LOW)
            return 0

        lax.fori_loop(0, rows // step, some, 0)
        stores += [
            pltpu.make_async_copy(part.at[i], whole.at[:, cols[i]], sems.at[6 + 2 * i + j])
            for j, (whole, part) in enumerate(((first_new, mn), (second_new, vn)))
        ]
        for store in stores[-2:]:
            store.start()
    for store in stores:
        store.wait()


def up(base, place, fixes, left, right, param, first, second, news):
    rows, width = left.shape
    ins = [place, fixes, left, right, param, first, second]
    in_specs = [SMEM, SMEM, VMEM, VMEM, HBM, HBM, HBM]
    aliases = {}
    if news is not None:
        aliases = {len(ins): 2, len(ins) + 1: 3}
        ins += news
        in_specs += [HBM] * 2
    return pl.pallas_call(
        partial(up_kernel, base),
        in_specs=in_specs,
        out_specs=[VMEM, VMEM, HBM, HBM],
        out_shape=[
            shape(2 * rows, width, dtype=WIDE),
            shape(2 * rows, width),
            shape(*param.shape, dtype=WIDE),
            shape(*param.shape, dtype=WIDE),
        ],
        scratch_shapes=[pltpu.VMEM((2, rows, width), WIDE)] * 5
        + [pltpu.SemaphoreType.DMA((10,))],
        input_output_aliases=aliases,
        compiler_params=params(),
        name="up",
    )(*ins)


def mean_down_kernel(local, *refs):
    out = refs[-1]
    for c in range(CHUNKS):
        cols = slice(STARTS[c], STARTS[c] + WIDTHS[c])
        out[:, cols] = 0.5 * (local[:, cols] + refs[c][...].astype(WIDE))


def mean_down(local, others):
    rows, cols = local.shape
    block = pl.BlockSpec((rows // 8, cols), lambda i: (i, 0))
    return pl.pallas_call(
        mean_down_kernel,
        grid=(8,),
        out_shape=shape(rows, cols, dtype=WIDE),
        in_specs=[block] + [pl.BlockSpec((rows // 8, w), lambda i: (i, 0)) for w in WIDTHS],
        out_specs=block,
        compiler_params=params(60 * 2**20),
        name="mean_down",
    )(local, *others)


def mean_up_kernel(base, place, local, other, *rest):
    out, kept, sems = rest[-3:]
    rows, width = kept.shape[1:]
    copies = []
    for i in range(2):
        kept[i] = 0.5 * (
            local[i * rows : (i + 1) * rows, :] + other[i * rows : (i + 1) * rows, :].astype(WIDE)
        )
        cols = pl.ds(pl.multiple_of((place[0] ^ (base + i)) * width, width), width)
        copies.append(pltpu.make_async_copy(kept.at[i], out.at[:, cols], sems.at[i]))
        copies[i].start()
    for copy in copies:
        copy.wait()


def mean_up(base, place, local, other, whole):
    rows, width = local.shape[0] // 2, local.shape[1]
    ins, in_specs, aliases = [place, local, other], [SMEM, VMEM, VMEM], {}
    if whole is not None:
        aliases = {3: 0}
        ins.append(whole)
        in_specs.append(HBM)
    return pl.pallas_call(
        partial(mean_up_kernel, base),
        in_specs=in_specs,
        out_specs=HBM,
        out_shape=shape(rows, 4 * width, dtype=WIDE),
        scratch_shapes=[pltpu.VMEM((2, rows, width), WIDE), pltpu.SemaphoreType.DMA((2,))],
        input_output_aliases=aliases,
        compiler_params=params(),
        name="mean_up",
    )(*ins)


def prepare(place, fixes, level, tokens, grads, up_p, down_p, down_m, down_v):
    first = cut(place, up_p, fixes, level)
    ups = [first[0]]
    for k in range(1, 4):
        ups.append(swap(first[k], k))
    n0, *own = norm(tokens, grads, first[0])
    n2 = swap(n0, 2)
    n1 = swap(n0, 1)
    side = swap(grads, 1)
    far, last = [], []
    for c in range(CHUNKS):
        far.append(swap(own[c], 2))
    near_act, near_slope = hidden(place, ups, n0, n1)
    n3 = swap(n2, 1)
    far_act, far_slope = hidden(place, ups, n2, n3)
    for c in range(CHUNKS):
        last.append(swap(far[c], 1))
    acts, slopes = (near_act, far_act), (near_slope, far_slope)
    news, sends = None, []
    for c in range(CHUNKS - 1):
        ogs = (own[c], side, far[c], last[c])
        *news, send = down(c, fixes, *acts, ogs, down_p, down_m, down_v, news, n0)
        sends.append(send)
    return news, sends, acts, slopes, own, side, far, last, (n0, n1, n2, n3)


def first_part(level, place, made, param):
    sends, slopes, own, side, far, last, normed = made
    others = []
    for send in sends:
        others.append(from_partner(send, 2**level))
    return others, back(place, param, slopes, own, side, far, last, normed)


def between(place, fixes, made, gs, up_p, down_p, up_m, down_m, up_v, down_v):
    news, acts, own, side, far, last = made
    g0, g1, g2, g3 = gs
    g2 = swap(g2, 2)
    g3 = swap(g3, 3)
    g1 = swap(g1, 1)
    c = CHUNKS - 1
    ogs = (own[c], side, far[c], last[c])
    *news, send = down(c, fixes, *acts, ogs, down_p, down_m, down_v, news, g0)
    near = up(0, place, fixes, g0, g1, up_p, up_m, up_v, None)
    return news, send, near, g2, g3


def finish(level, place, fixes, others, made, up_p, up_m, up_v):
    by = 2**level
    news, send, (near_local, near_send, *up_new), g2, g3 = made
    others = [*others, from_partner(send, by)]
    near_other = from_partner(near_send, by)
    far_local, send, *up_new = up(2, place, fixes, g2, g3, up_p, up_m, up_v, up_new)
    far_other = from_partner(send, by)
    new_down = mean_down(news[0], others)
    new_up = mean_up(0, place, near_local, near_other, None)
    new_up = mean_up(2, place, far_local, far_other, new_up)
    return new_up, new_down, up_new[0], news[1], up_new[1], news[2]


def body(tokens, out_grad, step, *state):
    levels = lax.axis_size("peer").bit_length() - 1
    place = lax.axis_index("zero").astype(jnp.int32)[None]
    state = [a[0] for a in state]
    count = (step[0] + 1).astype(WIDE)
    fixes = jnp.stack(
        [1.0 - jnp.power(WIDE(0.9), count), 1.0 - jnp.power(WIDE(0.999), count)]
    )
    level = step % levels
    news, sends, acts, slopes, own, side, far, last, normed = prepare(
        place, fixes, level, tokens[0], out_grad[0], state[0], *state[1::2]
    )

    def branch(part, k, *args):
        return part(k, *args)

    def switch(part, *args):
        return lax.switch(level[0], [partial(branch, part, k) for k in range(levels)], *args)

    others, gs = switch(first_part, place, (sends, slopes, own, side, far, last, normed), state[1])
    made = between(place, fixes, (news, acts, own, side, far, last), gs, *state)
    outs = switch(finish, place, fixes, others, made, *state[::2])
    return tuple(a[None] for a in outs)


def solution(mesh):
    in_specs = (P("peer", "zero", None), P("peer", "zero", None), P()) + (
        P("peer", "zero", None),
    ) * 6
    out_specs = (P("peer", "zero", None),) * 6
    return jax.shard_map(body, mesh=mesh, in_specs=in_specs, out_specs=out_specs, check_vma=False)
```

```python
from functools import partial

import jax
import jax.numpy as jnp
from jax import lax
from jax.experimental import pallas as pl
from jax.experimental.pallas import tpu as pltpu
from jax.sharding import PartitionSpec as P


WIDTHS = (384, 640)
STARTS = tuple(sum(WIDTHS[:c]) for c in range(len(WIDTHS)))
CHUNKS = len(WIDTHS)
LOW = jnp.bfloat16
WIDE = jnp.float32
VMEM = pl.BlockSpec(memory_space=pltpu.VMEM)
HBM = pl.BlockSpec(memory_space=pltpu.HBM)
ANY = pl.BlockSpec(memory_space=pl.ANY)
SMEM = pl.BlockSpec(memory_space=pltpu.SMEM)
LIMIT = 20 * 2**20


def shape(*sizes, dtype=LOW):
    return jax.ShapeDtypeStruct(sizes, dtype)


def params(limit=LIMIT):
    return pltpu.CompilerParams(vmem_limit_bytes=limit)


def swap(array, mask):
    size = lax.axis_size("zero")
    return lax.ppermute(array, "zero", [(i, i ^ mask) for i in range(size)])


def from_partner(array, by):
    size = lax.axis_size("peer")
    return lax.ppermute(array, "peer", [(i, (i - by) % size) for i in range(size)])


def dot(left, right, over=((1,), (0,))):
    return lax.dot_general(left, right, (over, ((), ())), preferred_element_type=WIDE)


def adam(param, first, second, grad, fixes):
    first_new = 0.9 * first + 0.1 * grad
    second_new = 0.999 * second + 0.001 * grad * grad
    scaled = first_new * (0.01 / fixes[0])
    local = param - scaled / (jnp.sqrt(second_new * (1.0 / fixes[1])) + 1e-08)
    return local, first_new, second_new


def cut_kernel(place, up, *refs):
    outs = refs[-4:]
    step = 32
    width = outs[0].shape[1]

    def rows(i, _):
        at = pl.ds(pl.multiple_of(i * step, step), step)
        for k in range(4):
            col = pl.multiple_of((place[0] ^ k) * width, width)
            outs[k][at, :] = up[at, pl.ds(col, width)].astype(LOW)
        return 0

    lax.fori_loop(0, up.shape[0] // step, rows, 0)


def cut(place, up, *after):
    return pl.pallas_call(
        cut_kernel,
        out_shape=[shape(up.shape[0], up.shape[1] // 4)] * 4,
        in_specs=[SMEM, VMEM] + [ANY] * len(after),
        out_specs=[VMEM] * 4,
        compiler_params=params(),
        name="cut",
    )(place, up, *after)


def pieces_kernel(grads, *refs):
    for c, piece in enumerate(refs[-CHUNKS:]):
        piece[...] = grads[:, STARTS[c] : STARTS[c] + WIDTHS[c]]


def pieces(grads, *after):
    return pl.pallas_call(
        pieces_kernel,
        out_shape=[shape(grads.shape[0], width) for width in WIDTHS],
        in_specs=[VMEM] + [ANY] * len(after),
        out_specs=[VMEM] * CHUNKS,
        compiler_params=params(),
        name="pieces",
    )(grads, *after)


def norm_kernel(tokens, _, normed):
    step = 64

    def rows(i, _):
        at = pl.ds(pl.multiple_of(i * step, step), step)
        wide = tokens[at, :].astype(WIDE)
        centered = wide - jnp.mean(wide, axis=1, keepdims=True)
        spread = jnp.mean(centered * centered, axis=1, keepdims=True)
        normed[at, :] = (centered * lax.rsqrt(spread + 1e-05)).astype(LOW)
        return 0

    lax.fori_loop(0, tokens.shape[0] // step, rows, 0)


def norm(tokens, after):
    return pl.pallas_call(
        norm_kernel,
        out_shape=shape(*tokens.shape),
        in_specs=[VMEM, ANY],
        out_specs=VMEM,
        compiler_params=params(),
        name="norm",
    )(tokens, after)


def hidden_kernel(place, u0, u1, u2, u3, left, right, act, slope, up, both):
    size = u0.shape[0]
    for k, u in enumerate((u0, u1, u2, u3)):
        up[pl.ds(pl.multiple_of((place[0] ^ k) * size, size), size), :] = u[...]
    half = left.shape[0]
    both[:half, :] = left[...]
    both[half:, :] = right[...]
    step = 256

    def rows(i, _):
        at = pl.ds(pl.multiple_of(i * step, step), step)
        pre = dot(both[at, :], up[...])
        square = pre * pre
        bent = jnp.tanh(0.7978845608 * (pre + 0.044715 * square * pre))
        lift = 0.5 * (1.0 + bent)
        act[:, at] = (pre * lift).T.astype(LOW)
        slope[at, :] = lift + 0.5 * pre * (1.0 - bent * bent) * (
            0.7978845608 + 0.1070322243 * square
        )
        return 0

    lax.fori_loop(0, 2 * half // step, rows, 0)


def hidden(place, ups, left, right):
    rows, full = left.shape
    width = ups[0].shape[1]
    return pl.pallas_call(
        hidden_kernel,
        out_shape=[shape(width, 2 * rows), shape(2 * rows, width, dtype=WIDE)],
        in_specs=[SMEM] + [VMEM] * 6,
        out_specs=[VMEM] * 2,
        scratch_shapes=[pltpu.VMEM((full, width), LOW), pltpu.VMEM((2 * rows, full), LOW)],
        compiler_params=params(),
        name="hidden",
    )(place, *ups, left, right)


def down_kernel(c, fixes, near, far, o0, o1, o2, o3, param, first, second, *rest):
    wholes, kept, (p, m, v, sems) = rest[-12:-8], rest[-8:-4], rest[-4:]
    local, send, mn, vn = kept
    cols = pl.ds(STARTS[c], WIDTHS[c])
    loads = [
        pltpu.make_async_copy(whole.at[:, cols], part, sems.at[i])
        for i, (whole, part) in enumerate(((param, p), (first, m), (second, v)))
    ]
    for load in loads:
        load.start()
    rows = o0.shape[0]
    local[...] = dot(near[:, :rows], o0[...])
    local[...] += dot(near[:, rows:], o1[:, STARTS[c] : STARTS[c] + WIDTHS[c]])
    local[...] += dot(far[:, :rows], o2[...])
    local[...] += dot(far[:, rows:], o3[...])
    for load in loads:
        load.wait()
    step = 64

    def some(i, _):
        at = pl.ds(pl.multiple_of(i * step, step), step)
        after, mn[at, :], vn[at, :] = adam(p[at, :], m[at, :], v[at, :], local[at, :], fixes)
        local[at, :] = after
        send[at, :] = after.astype(LOW)
        return 0

    lax.fori_loop(0, rows // step, some, 0)
    stores = [
        pltpu.make_async_copy(part, whole.at[:, cols], sems.at[i])
        for i, (whole, part) in enumerate(zip(wholes, kept))
    ]
    for store in stores:
        store.start()
    for store in stores:
        store.wait()


def down(c, fixes, near, far, ogs, param, first, second, news, after):
    rows, cols = param.shape
    part = (rows, WIDTHS[c])
    ins = [fixes, near, far, *ogs, param, first, second, after]
    in_specs = [SMEM] + [VMEM] * 6 + [HBM] * 3 + [ANY]
    aliases = {}
    if news is not None:
        aliases = {len(ins) + i: i for i in range(4)}
        ins += news
        in_specs += [HBM] * 4
    kinds = (WIDE, LOW, WIDE, WIDE)
    return pl.pallas_call(
        partial(down_kernel, c),
        out_shape=[shape(rows, cols, dtype=kind) for kind in kinds],
        in_specs=in_specs,
        out_specs=[HBM] * 4,
        input_output_aliases=aliases,
        scratch_shapes=[pltpu.VMEM(part, kind) for kind in kinds + (WIDE,) * 3]
        + [pltpu.SemaphoreType.DMA((4,))],
        compiler_params=params(),
        name="down",
    )(*ins)


def back_kernel(place, param, sa, sb, *refs):
    ogs, side, outs = refs[: 3 * CHUNKS], refs[3 * CHUNKS], refs[-4:-2]
    normed = refs[3 * CHUNKS + 1 : 3 * CHUNKS + 5]
    pre_grad, low = refs[-2:]
    rows = normed[0].shape[0]
    low[...] = param[...].astype(LOW)
    for k in range(4):
        got = None
        for c in range(CHUNKS):
            cols = slice(STARTS[c], STARTS[c] + WIDTHS[c])
            piece = side[:, cols] if k == 1 else ogs[(0, 0, 1, 2)[k] * CHUNKS + c][...]
            part = dot(piece, low[:, cols], ((1,), (1,)))
            got = part if got is None else got + part
        slope = (sa, sb)[k // 2][(k % 2) * rows : (k % 2 + 1) * rows, :]
        pre_grad[k * rows : (k + 1) * rows, :] = (got * slope).astype(LOW)
    blocks(place, (2, 3), normed, pre_grad, outs)


def blocks(place, masks, normed, pre_grad, outs):
    rows = normed[0].shape[0]
    size = outs[0].shape[0]
    for k, out in zip(masks, outs):
        at = pl.ds(pl.multiple_of((place[0] ^ k) * size, size), size)
        total = None
        for j in range(4):
            part = dot(normed[j][:, at], pre_grad[j * rows : (j + 1) * rows, :], ((0,), (0,)))
            total = part if total is None else total + part
        out[...] = total.astype(LOW)


def rest_kernel(place, *refs):
    blocks(place, (0, 1), refs[:4], refs[4], refs[5:])


def rest_of_back(place, normed, pre_grad):
    size, hidden_size = normed[0].shape[1] // 4, pre_grad.shape[1]
    return pl.pallas_call(
        rest_kernel,
        out_shape=[shape(size, hidden_size)] * 2,
        in_specs=[SMEM] + [VMEM] * 5,
        out_specs=[VMEM] * 2,
        compiler_params=params(),
        name="rest",
    )(place, *normed, pre_grad)


def back(place, param, slopes, own, side, far, last, normed):
    hidden_size = param.shape[0]
    rows, full = normed[0].shape
    return pl.pallas_call(
        back_kernel,
        out_shape=[shape(full // 4, hidden_size)] * 2 + [shape(4 * rows, hidden_size)],
        in_specs=[SMEM] + [VMEM] * (3 + 3 * CHUNKS + 5),
        out_specs=[VMEM] * 3,
        scratch_shapes=[pltpu.VMEM(param.shape, LOW)],
        compiler_params=params(),
        name="back",
    )(place, param, *slopes, *own, *far, *last, side, *normed)


def up_kernel(base, place, fixes, left, right, param, first, second, *rest):
    local, send, first_new, second_new, p, m, v, mn, vn, sems = rest[-10:]
    rows, width = left.shape
    cols = [
        pl.ds(pl.multiple_of((place[0] ^ (base + i)) * width, width), width) for i in range(2)
    ]
    loads = [
        [
            pltpu.make_async_copy(whole.at[:, cols[i]], part.at[i], sems.at[3 * i + j])
            for j, (whole, part) in enumerate(((param, p), (first, m), (second, v)))
        ]
        for i in range(2)
    ]
    for load in loads[0] + loads[1]:
        load.start()
    stores = []
    step = 32
    for i, grads in enumerate((left, right)):
        for load in loads[i]:
            load.wait()

        def some(r, _):
            at = pl.ds(pl.multiple_of(r * step, step), step)
            to = pl.ds(pl.multiple_of(i * rows + r * step, step), step)
            after, mn[i, at, :], vn[i, at, :] = adam(
                p[i, at, :], m[i, at, :], v[i, at, :], grads[at, :].astype(WIDE), fixes
            )
            local[to, :] = after
            send[to, :] = after.astype(LOW)
            return 0

        lax.fori_loop(0, rows // step, some, 0)
        stores += [
            pltpu.make_async_copy(part.at[i], whole.at[:, cols[i]], sems.at[6 + 2 * i + j])
            for j, (whole, part) in enumerate(((first_new, mn), (second_new, vn)))
        ]
        for store in stores[-2:]:
            store.start()
    for store in stores:
        store.wait()


def up(base, place, fixes, left, right, param, first, second, news):
    rows, width = left.shape
    ins = [place, fixes, left, right, param, first, second]
    in_specs = [SMEM, SMEM, VMEM, VMEM, HBM, HBM, HBM]
    aliases = {}
    if news is not None:
        aliases = {len(ins): 2, len(ins) + 1: 3}
        ins += news
        in_specs += [HBM] * 2
    return pl.pallas_call(
        partial(up_kernel, base),
        in_specs=in_specs,
        out_specs=[VMEM, VMEM, HBM, HBM],
        out_shape=[
            shape(2 * rows, width, dtype=WIDE),
            shape(2 * rows, width),
            shape(*param.shape, dtype=WIDE),
            shape(*param.shape, dtype=WIDE),
        ],
        scratch_shapes=[pltpu.VMEM((2, rows, width), WIDE)] * 5
        + [pltpu.SemaphoreType.DMA((10,))],
        input_output_aliases=aliases,
        compiler_params=params(),
        name="up",
    )(*ins)


def mean_down_kernel(local, other, out):
    out[...] = 0.5 * (local[...] + other[...].astype(WIDE))


def mean_down(local, other):
    rows, cols = local.shape
    block = pl.BlockSpec((rows // 8, cols), lambda i: (i, 0))
    return pl.pallas_call(
        mean_down_kernel,
        grid=(8,),
        out_shape=shape(rows, cols, dtype=WIDE),
        in_specs=[block] * 2,
        out_specs=block,
        compiler_params=params(60 * 2**20),
        name="mean_down",
    )(local, other)


def mean_up_kernel(base, place, local, other, *rest):
    out, kept, sems = rest[-3:]
    rows, width = kept.shape[1:]
    copies = []
    for i in range(2):
        kept[i] = 0.5 * (
            local[i * rows : (i + 1) * rows, :] + other[i * rows : (i + 1) * rows, :].astype(WIDE)
        )
        cols = pl.ds(pl.multiple_of((place[0] ^ (base + i)) * width, width), width)
        copies.append(pltpu.make_async_copy(kept.at[i], out.at[:, cols], sems.at[i]))
        copies[i].start()
    for copy in copies:
        copy.wait()


def mean_up(base, place, local, other, whole):
    rows, width = local.shape[0] // 2, local.shape[1]
    ins, in_specs, aliases = [place, local, other], [SMEM, VMEM, VMEM], {}
    if whole is not None:
        aliases = {3: 0}
        ins.append(whole)
        in_specs.append(HBM)
    return pl.pallas_call(
        partial(mean_up_kernel, base),
        in_specs=in_specs,
        out_specs=HBM,
        out_shape=shape(rows, 4 * width, dtype=WIDE),
        scratch_shapes=[pltpu.VMEM((2, rows, width), WIDE), pltpu.SemaphoreType.DMA((2,))],
        input_output_aliases=aliases,
        compiler_params=params(),
        name="mean_up",
    )(*ins)


def prepare(place, fixes, level, tokens, grads, up_p, down_p, up_m, down_m, up_v, down_v):
    own = pieces(grads, fixes, level)
    first = cut(place, up_p, own[0])
    ups = [first[0]]
    for k in range(1, 4):
        ups.append(swap(first[k], k))
    n0 = norm(tokens, first[0])
    n2 = swap(n0, 2)
    n1 = swap(n0, 1)
    side = swap(grads, 1)
    far, last = [], []
    for c in range(CHUNKS):
        far.append(swap(own[c], 2))
    near_act, near_slope = hidden(place, ups, n0, n1)
    n3 = swap(n2, 1)
    far_act, far_slope = hidden(place, ups, n2, n3)
    for c in range(CHUNKS):
        last.append(swap(far[c], 1))
    acts, slopes = (near_act, far_act), (near_slope, far_slope)
    news = None
    for c in range(CHUNKS - 1):
        ogs = (own[c], side, far[c], last[c])
        news = down(c, fixes, *acts, ogs, down_p, down_m, down_v, news, n0)
    normed = (n0, n1, n2, n3)
    g2, g3, pre_grad = back(place, down_p, slopes, own, side, far, last, normed)
    g2 = swap(g2, 2)
    g3 = swap(g3, 3)
    g0, g1 = rest_of_back(place, normed, pre_grad)
    g1 = swap(g1, 1)
    c = CHUNKS - 1
    ogs = (own[c], side, far[c], last[c])
    news = down(c, fixes, *acts, ogs, down_p, down_m, down_v, news, g0)
    near = up(0, place, fixes, g0, g1, up_p, up_m, up_v, None)
    return news, near, g2, g3


def finish(level, place, fixes, made, up_p, up_m, up_v):
    by = 2**level
    (down_local, send, *down_new), (near_local, near_send, *up_new), g2, g3 = made
    other = from_partner(send, by)
    near_other = from_partner(near_send, by)
    far_local, send, *up_new = up(2, place, fixes, g2, g3, up_p, up_m, up_v, up_new)
    far_other = from_partner(send, by)
    new_down = mean_down(down_local, other)
    new_up = mean_up(0, place, near_local, near_other, None)
    new_up = mean_up(2, place, far_local, far_other, new_up)
    return new_up, new_down, up_new[0], down_new[0], up_new[1], down_new[1]


def body(tokens, out_grad, step, *state):
    levels = lax.axis_size("peer").bit_length() - 1
    place = lax.axis_index("zero").astype(jnp.int32)[None]
    state = [a[0] for a in state]
    count = (step[0] + 1).astype(WIDE)
    fixes = jnp.stack(
        [1.0 - jnp.power(WIDE(0.9), count), 1.0 - jnp.power(WIDE(0.999), count)]
    )
    level = step % levels
    made = prepare(place, fixes, level, tokens[0], out_grad[0], *state)

    def branch(k, *args):
        return finish(k, *args)

    outs = lax.switch(
        level[0],
        [partial(branch, k) for k in range(levels)],
        place,
        fixes,
        made,
        *state[::2],
    )
    return tuple(a[None] for a in outs)


def solution(mesh):
    in_specs = (P("peer", "zero", None), P("peer", "zero", None), P()) + (
        P("peer", "zero", None),
    ) * 6
    out_specs = (P("peer", "zero", None),) * 6
    return jax.shard_map(body, mesh=mesh, in_specs=in_specs, out_specs=out_specs, check_vma=False)
```

```python
from functools import partial

import jax
import jax.numpy as jnp
from jax import lax
from jax.experimental import pallas as pl
from jax.experimental.pallas import tpu as pltpu
from jax.sharding import PartitionSpec as P


WIDTHS = (512, 512)
STARTS = tuple(sum(WIDTHS[:c]) for c in range(len(WIDTHS)))
CHUNKS = len(WIDTHS)
LOW = jnp.bfloat16
WIDE = jnp.float32
VMEM = pl.BlockSpec(memory_space=pltpu.VMEM)
HBM = pl.BlockSpec(memory_space=pltpu.HBM)
ANY = pl.BlockSpec(memory_space=pl.ANY)
SMEM = pl.BlockSpec(memory_space=pltpu.SMEM)
LIMIT = 20 * 2**20


def shape(*sizes, dtype=LOW):
    return jax.ShapeDtypeStruct(sizes, dtype)


def params(limit=LIMIT):
    return pltpu.CompilerParams(vmem_limit_bytes=limit)


def swap(array, mask):
    size = lax.axis_size("zero")
    return lax.ppermute(array, "zero", [(i, i ^ mask) for i in range(size)])


def from_partner(array, by):
    size = lax.axis_size("peer")
    return lax.ppermute(array, "peer", [(i, (i - by) % size) for i in range(size)])


def dot(left, right, over=((1,), (0,))):
    return lax.dot_general(left, right, (over, ((), ())), preferred_element_type=WIDE)


def adam(param, first, second, grad, fixes):
    first_new = 0.9 * first + 0.1 * grad
    second_new = 0.999 * second + 0.001 * grad * grad
    scaled = first_new * (0.01 / fixes[0])
    local = param - scaled / (jnp.sqrt(second_new * (1.0 / fixes[1])) + 1e-08)
    return local, first_new, second_new


def cut_kernel(place, up, *refs):
    outs = refs[-4:]
    step = 32
    width = outs[0].shape[1]

    def rows(i, _):
        at = pl.ds(pl.multiple_of(i * step, step), step)
        for k in range(4):
            col = pl.multiple_of((place[0] ^ k) * width, width)
            outs[k][at, :] = up[at, pl.ds(col, width)].astype(LOW)
        return 0

    lax.fori_loop(0, up.shape[0] // step, rows, 0)


def cut(place, up, *after):
    return pl.pallas_call(
        cut_kernel,
        out_shape=[shape(up.shape[0], up.shape[1] // 4)] * 4,
        in_specs=[SMEM, VMEM] + [ANY] * len(after),
        out_specs=[VMEM] * 4,
        compiler_params=params(),
        name="cut",
    )(place, up, *after)


def pieces_kernel(grads, *refs):
    for c, piece in enumerate(refs[-CHUNKS:]):
        piece[...] = grads[:, STARTS[c] : STARTS[c] + WIDTHS[c]]


def pieces(grads, *after):
    return pl.pallas_call(
        pieces_kernel,
        out_shape=[shape(grads.shape[0], width) for width in WIDTHS],
        in_specs=[VMEM] + [ANY] * len(after),
        out_specs=[VMEM] * CHUNKS,
        compiler_params=params(),
        name="pieces",
    )(grads, *after)


def norm_kernel(tokens, _, normed):
    step = 64

    def rows(i, _):
        at = pl.ds(pl.multiple_of(i * step, step), step)
        wide = tokens[at, :].astype(WIDE)
        centered = wide - jnp.mean(wide, axis=1, keepdims=True)
        spread = jnp.mean(centered * centered, axis=1, keepdims=True)
        normed[at, :] = (centered * lax.rsqrt(spread + 1e-05)).astype(LOW)
        return 0

    lax.fori_loop(0, tokens.shape[0] // step, rows, 0)


def norm(tokens, after):
    return pl.pallas_call(
        norm_kernel,
        out_shape=shape(*tokens.shape),
        in_specs=[VMEM, ANY],
        out_specs=VMEM,
        compiler_params=params(),
        name="norm",
    )(tokens, after)


def hidden_kernel(place, u0, u1, u2, u3, left, right, act, slope, up, both):
    size = u0.shape[0]
    for k, u in enumerate((u0, u1, u2, u3)):
        up[pl.ds(pl.multiple_of((place[0] ^ k) * size, size), size), :] = u[...]
    half = left.shape[0]
    both[:half, :] = left[...]
    both[half:, :] = right[...]
    step = 256

    def rows(i, _):
        at = pl.ds(pl.multiple_of(i * step, step), step)
        pre = dot(both[at, :], up[...])
        square = pre * pre
        bent = jnp.tanh(0.7978845608 * (pre + 0.044715 * square * pre))
        lift = 0.5 * (1.0 + bent)
        act[:, at] = (pre * lift).T.astype(LOW)
        slope[at, :] = lift + 0.5 * pre * (1.0 - bent * bent) * (
            0.7978845608 + 0.1070322243 * square
        )
        return 0

    lax.fori_loop(0, 2 * half // step, rows, 0)


def hidden(place, ups, left, right):
    rows, full = left.shape
    width = ups[0].shape[1]
    return pl.pallas_call(
        hidden_kernel,
        out_shape=[shape(width, 2 * rows), shape(2 * rows, width, dtype=WIDE)],
        in_specs=[SMEM] + [VMEM] * 6,
        out_specs=[VMEM] * 2,
        scratch_shapes=[pltpu.VMEM((full, width), LOW), pltpu.VMEM((2 * rows, full), LOW)],
        compiler_params=params(),
        name="hidden",
    )(place, *ups, left, right)


def down_kernel(c, fixes, near, far, o0, o1, o2, o3, param, first, second, *rest):
    wholes, kept, (p, m, v, sems) = rest[-12:-8], rest[-8:-4], rest[-4:]
    local, send, mn, vn = kept
    cols = pl.ds(STARTS[c], WIDTHS[c])
    loads = [
        pltpu.make_async_copy(whole.at[:, cols], part, sems.at[i])
        for i, (whole, part) in enumerate(((param, p), (first, m), (second, v)))
    ]
    for load in loads:
        load.start()
    rows = o0.shape[0]
    local[...] = dot(near[:, :rows], o0[...])
    local[...] += dot(near[:, rows:], o1[:, STARTS[c] : STARTS[c] + WIDTHS[c]])
    local[...] += dot(far[:, :rows], o2[...])
    local[...] += dot(far[:, rows:], o3[...])
    for load in loads:
        load.wait()
    step = 64

    def some(i, _):
        at = pl.ds(pl.multiple_of(i * step, step), step)
        after, mn[at, :], vn[at, :] = adam(p[at, :], m[at, :], v[at, :], local[at, :], fixes)
        local[at, :] = after
        send[at, :] = after.astype(LOW)
        return 0

    lax.fori_loop(0, rows // step, some, 0)
    stores = [
        pltpu.make_async_copy(part, whole.at[:, cols], sems.at[i])
        for i, (whole, part) in enumerate(zip(wholes, kept))
    ]
    for store in stores:
        store.start()
    for store in stores:
        store.wait()


def down(c, fixes, near, far, ogs, param, first, second, news, after):
    rows, cols = param.shape
    part = (rows, WIDTHS[c])
    ins = [fixes, near, far, *ogs, param, first, second, after]
    in_specs = [SMEM] + [VMEM] * 6 + [HBM] * 3 + [ANY]
    aliases = {}
    if news is not None:
        aliases = {len(ins) + i: i for i in range(4)}
        ins += news
        in_specs += [HBM] * 4
    kinds = (WIDE, LOW, WIDE, WIDE)
    return pl.pallas_call(
        partial(down_kernel, c),
        out_shape=[shape(rows, cols, dtype=kind) for kind in kinds],
        in_specs=in_specs,
        out_specs=[HBM] * 4,
        input_output_aliases=aliases,
        scratch_shapes=[pltpu.VMEM(part, kind) for kind in kinds + (WIDE,) * 3]
        + [pltpu.SemaphoreType.DMA((4,))],
        compiler_params=params(),
        name="down",
    )(*ins)


def lower_kernel(param, low):
    low[...] = param[...].astype(LOW)


def lower(param):
    return pl.pallas_call(
        lower_kernel,
        out_shape=shape(*param.shape),
        in_specs=[VMEM],
        out_specs=VMEM,
        compiler_params=params(),
        name="lower",
    )(param)


def back_kernel(place, low, sa, sb, *refs):
    ogs, side, outs = refs[: 3 * CHUNKS], refs[3 * CHUNKS], refs[-3:-1]
    normed = refs[3 * CHUNKS + 1 : 3 * CHUNKS + 5]
    pre_grad = refs[-1]
    rows = normed[0].shape[0]
    for k in range(4):
        got = None
        for c in range(CHUNKS):
            cols = slice(STARTS[c], STARTS[c] + WIDTHS[c])
            piece = side[:, cols] if k == 1 else ogs[(0, 0, 1, 2)[k] * CHUNKS + c][...]
            part = dot(piece, low[:, cols], ((1,), (1,)))
            got = part if got is None else got + part
        slope = (sa, sb)[k // 2][(k % 2) * rows : (k % 2 + 1) * rows, :]
        pre_grad[k * rows : (k + 1) * rows, :] = (got * slope).astype(LOW)
    blocks(place, (2, 3), normed, pre_grad, outs)


def blocks(place, masks, normed, pre_grad, outs):
    rows = normed[0].shape[0]
    size = outs[0].shape[0]
    for k, out in zip(masks, outs):
        at = pl.ds(pl.multiple_of((place[0] ^ k) * size, size), size)
        total = None
        for j in range(4):
            part = dot(normed[j][:, at], pre_grad[j * rows : (j + 1) * rows, :], ((0,), (0,)))
            total = part if total is None else total + part
        out[...] = total.astype(LOW)


def rest_kernel(place, *refs):
    blocks(place, (0, 1), refs[:4], refs[4], refs[5:])


def rest_of_back(place, normed, pre_grad):
    size, hidden_size = normed[0].shape[1] // 4, pre_grad.shape[1]
    return pl.pallas_call(
        rest_kernel,
        out_shape=[shape(size, hidden_size)] * 2,
        in_specs=[SMEM] + [VMEM] * 5,
        out_specs=[VMEM] * 2,
        compiler_params=params(),
        name="rest",
    )(place, *normed, pre_grad)


def back(place, param, slopes, own, side, far, last, normed):
    hidden_size = param.shape[0]
    rows, full = normed[0].shape
    return pl.pallas_call(
        back_kernel,
        out_shape=[shape(full // 4, hidden_size)] * 2 + [shape(4 * rows, hidden_size)],
        in_specs=[SMEM] + [VMEM] * (3 + 3 * CHUNKS + 5),
        out_specs=[VMEM] * 3,
        compiler_params=params(),
        name="back",
    )(place, param, *slopes, *own, *far, *last, side, *normed)


def up_kernel(base, place, fixes, left, right, param, first, second, *rest):
    local, send, first_new, second_new, p, m, v, mn, vn, sems = rest[-10:]
    rows, width = left.shape
    cols = [
        pl.ds(pl.multiple_of((place[0] ^ (base + i)) * width, width), width) for i in range(2)
    ]
    loads = [
        [
            pltpu.make_async_copy(whole.at[:, cols[i]], part.at[i], sems.at[3 * i + j])
            for j, (whole, part) in enumerate(((param, p), (first, m), (second, v)))
        ]
        for i in range(2)
    ]
    for load in loads[0] + loads[1]:
        load.start()
    stores = []
    step = 32
    for i, grads in enumerate((left, right)):
        for load in loads[i]:
            load.wait()

        def some(r, _):
            at = pl.ds(pl.multiple_of(r * step, step), step)
            to = pl.ds(pl.multiple_of(i * rows + r * step, step), step)
            after, mn[i, at, :], vn[i, at, :] = adam(
                p[i, at, :], m[i, at, :], v[i, at, :], grads[at, :].astype(WIDE), fixes
            )
            local[to, :] = after
            send[to, :] = after.astype(LOW)
            return 0

        lax.fori_loop(0, rows // step, some, 0)
        stores += [
            pltpu.make_async_copy(part.at[i], whole.at[:, cols[i]], sems.at[6 + 2 * i + j])
            for j, (whole, part) in enumerate(((first_new, mn), (second_new, vn)))
        ]
        for store in stores[-2:]:
            store.start()
    for store in stores:
        store.wait()


def up(base, place, fixes, left, right, param, first, second, news):
    rows, width = left.shape
    ins = [place, fixes, left, right, param, first, second]
    in_specs = [SMEM, SMEM, VMEM, VMEM, HBM, HBM, HBM]
    aliases = {}
    if news is not None:
        aliases = {len(ins): 2, len(ins) + 1: 3}
        ins += news
        in_specs += [HBM] * 2
    return pl.pallas_call(
        partial(up_kernel, base),
        in_specs=in_specs,
        out_specs=[VMEM, VMEM, HBM, HBM],
        out_shape=[
            shape(2 * rows, width, dtype=WIDE),
            shape(2 * rows, width),
            shape(*param.shape, dtype=WIDE),
            shape(*param.shape, dtype=WIDE),
        ],
        scratch_shapes=[pltpu.VMEM((2, rows, width), WIDE)] * 5
        + [pltpu.SemaphoreType.DMA((10,))],
        input_output_aliases=aliases,
        compiler_params=params(),
        name="up",
    )(*ins)


def mean_down_kernel(local, other, out):
    out[...] = 0.5 * (local[...] + other[...].astype(WIDE))


def mean_down(local, other):
    rows, cols = local.shape
    block = pl.BlockSpec((rows // 8, cols), lambda i: (i, 0))
    return pl.pallas_call(
        mean_down_kernel,
        grid=(8,),
        out_shape=shape(rows, cols, dtype=WIDE),
        in_specs=[block] * 2,
        out_specs=block,
        compiler_params=params(60 * 2**20),
        name="mean_down",
    )(local, other)


def mean_up_kernel(base, place, local, other, *rest):
    out, kept, sems = rest[-3:]
    rows, width = kept.shape[1:]
    copies = []
    for i in range(2):
        kept[i] = 0.5 * (
            local[i * rows : (i + 1) * rows, :] + other[i * rows : (i + 1) * rows, :].astype(WIDE)
        )
        cols = pl.ds(pl.multiple_of((place[0] ^ (base + i)) * width, width), width)
        copies.append(pltpu.make_async_copy(kept.at[i], out.at[:, cols], sems.at[i]))
        copies[i].start()
    for copy in copies:
        copy.wait()


def mean_up(base, place, local, other, whole):
    rows, width = local.shape[0] // 2, local.shape[1]
    ins, in_specs, aliases = [place, local, other], [SMEM, VMEM, VMEM], {}
    if whole is not None:
        aliases = {3: 0}
        ins.append(whole)
        in_specs.append(HBM)
    return pl.pallas_call(
        partial(mean_up_kernel, base),
        in_specs=in_specs,
        out_specs=HBM,
        out_shape=shape(rows, 4 * width, dtype=WIDE),
        scratch_shapes=[pltpu.VMEM((2, rows, width), WIDE), pltpu.SemaphoreType.DMA((2,))],
        input_output_aliases=aliases,
        compiler_params=params(),
        name="mean_up",
    )(*ins)


def prepare(place, fixes, level, tokens, grads, up_p, down_p, up_m, down_m, up_v, down_v):
    own = pieces(grads)
    first = cut(place, up_p, own[0], fixes, level)
    ups = [first[0]]
    for k in range(1, 4):
        ups.append(swap(first[k], k))
    n0 = norm(tokens, first[0])
    n2 = swap(n0, 2)
    n1 = swap(n0, 1)
    side = swap(grads, 1)
    far, last = [], []
    for c in range(CHUNKS):
        far.append(swap(own[c], 2))
    near_act, near_slope = hidden(place, ups, n0, n1)
    down_low = lower(down_p)
    n3 = swap(n2, 1)
    far_act, far_slope = hidden(place, ups, n2, n3)
    for c in range(CHUNKS):
        last.append(swap(far[c], 1))
    acts, slopes = (near_act, far_act), (near_slope, far_slope)
    news = None
    for c in range(CHUNKS - 1):
        ogs = (own[c], side, far[c], last[c])
        news = down(c, fixes, *acts, ogs, down_p, down_m, down_v, news, n0)
    normed = (n0, n1, n2, n3)
    g2, g3, pre_grad = back(place, down_low, slopes, own, side, far, last, normed)
    g2 = swap(g2, 2)
    g3 = swap(g3, 3)
    g0, g1 = rest_of_back(place, normed, pre_grad)
    g1 = swap(g1, 1)
    c = CHUNKS - 1
    ogs = (own[c], side, far[c], last[c])
    news = down(c, fixes, *acts, ogs, down_p, down_m, down_v, news, g0)
    near = up(0, place, fixes, g0, g1, up_p, up_m, up_v, None)
    return news, near, g2, g3


def finish(level, place, fixes, made, up_p, up_m, up_v):
    by = 2**level
    (down_local, send, *down_new), (near_local, near_send, *up_new), g2, g3 = made
    other = from_partner(send, by)
    near_other = from_partner(near_send, by)
    far_local, send, *up_new = up(2, place, fixes, g2, g3, up_p, up_m, up_v, up_new)
    far_other = from_partner(send, by)
    new_down = mean_down(down_local, other)
    new_up = mean_up(0, place, near_local, near_other, None)
    new_up = mean_up(2, place, far_local, far_other, new_up)
    return new_up, new_down, up_new[0], down_new[0], up_new[1], down_new[1]


def body(tokens, out_grad, step, *state):
    levels = lax.axis_size("peer").bit_length() - 1
    place = lax.axis_index("zero").astype(jnp.int32)[None]
    state = [a[0] for a in state]
    count = (step[0] + 1).astype(WIDE)
    fixes = jnp.stack(
        [1.0 - jnp.power(WIDE(0.9), count), 1.0 - jnp.power(WIDE(0.999), count)]
    )
    level = step % levels
    made = prepare(place, fixes, level, tokens[0], out_grad[0], *state)

    def branch(k, *args):
        return finish(k, *args)

    outs = lax.switch(
        level[0],
        [partial(branch, k) for k in range(levels)],
        place,
        fixes,
        made,
        *state[::2],
    )
    return tuple(a[None] for a in outs)


def solution(mesh):
    in_specs = (P("peer", "zero", None), P("peer", "zero", None), P()) + (
        P("peer", "zero", None),
    ) * 6
    out_specs = (P("peer", "zero", None),) * 6
    return jax.shard_map(body, mesh=mesh, in_specs=in_specs, out_specs=out_specs, check_vma=False)
```
